128 devices in a mesh: grp: 4 (over z), cell: 32 (over x, y, core).
Axes of the slice: x: 4, y: 4, z: 4, core: 2. Of those that a mesh axis runs over, the one named last changes fastest.
Arguments:
- load: float32 [128, 2048, 256], P(('grp', 'cell')), may hold values from -6 to 6
- schur: bfloat16 [128, 2048, 2048], P(('grp', 'cell')), as said below
- local_inverse: bfloat16 [128, 2048, 2048], P(('grp', 'cell')), as said below
- face_map: int32 [128, 4, 512], P(('grp', 'cell')), may hold values from 0 to 511, as said below
- primal_basis: bfloat16 [128, 32, 2048], P(('grp', 'cell')), may hold values from -0.25 to 0.25
- primal_index: int32 [128, 32], P(('grp', 'cell')), may hold values from 0 to 1023
- group_inverse: float32 [4, 1024, 1024], P('grp', 'cell'), as said below
- group_to_coarsest: float32 [4, 1024, 128], P('grp', 'cell'), may hold values from -0.1875 to 0.1875
- coarsest_inverse: float32 [128, 128], replicated, as said below
Outputs:
- solution: float32 [128, 2048, 256], P(('grp', 'cell'))
- residual: float32 [128, 2048, 256], P(('grp', 'cell'))
The draws below stay inside these ranges and needn't reach their ends.
Inputs may be any that keep to these rules, and one draw needn't show every extreme that they name: face_map[i, f] is a permutation of 0 .. 511, and the maps of two neighbouring cells across their shared face are inverse to each other. `schur`: each cell's matrix is symmetric positive definite. `local_inverse`: each cell's matrix is symmetric positive definite. `group_inverse`: each row's matrix is symmetric positive definite. `coarsest_inverse`: symmetric positive definite.
All inputs are finite; a program needn't handle non-finite values.
Results may differ from the reference program's by a relative error of at most 0.0066.
Values sent between devices are 32-bit elements; how exact they have to be, the bound alone decides.
A program may use at most 128 MiB of HBM per device.

```python
import math
import jax
import jax.numpy as jnp
from jax import lax

IFACE = 2048
FACE = 512
RHS = 256
PRIM = 32
NQ = 128
ITERS = 2
LAT_ROWS = 4
LAT_COLS = 32
CELLS = 128
NCG = 1024


def one_definite(key, order, center, spread):
    noise = jax.random.normal(jax.random.fold_in(key, 1), (order, order), jnp.float32)
    matrix = (noise + noise.T) * (spread / math.sqrt(2.0 * order)) + center * jnp.eye(order, dtype=jnp.float32)
    return matrix


def stack_definite(key, count, order, center, spread):
    keys = jax.random.split(key, count)
    return lax.map(lambda single: one_definite(single, order, center, spread), keys)


def draw_schur(key, part):
    return stack_definite(jax.random.fold_in(key, 11), CELLS, IFACE, 2.0, 0.6).astype(jnp.bfloat16)


def draw_local_inverse(key, part):
    return stack_definite(jax.random.fold_in(key, 12), CELLS, IFACE, 0.5, 0.15).astype(jnp.bfloat16)


def draw_group_inverse(key, part):
    return stack_definite(jax.random.fold_in(key, 13), LAT_ROWS, NCG, 1.0, 0.3)


def draw_coarsest_inverse(key, part):
    return stack_definite(jax.random.fold_in(key, 14), 1, NQ, 0.5, 0.15)[0]


def draw_face_map(key, part):
    keys = jax.random.split(jax.random.fold_in(key, 15), 4 * CELLS)
    perms = jax.vmap(lambda single: jax.random.permutation(single, FACE))(keys).astype(jnp.int32)
    across = perms[:CELLS].reshape(LAT_ROWS, LAT_COLS, FACE)
    upward = perms[CELLS:2 * CELLS].reshape(LAT_ROWS, LAT_COLS, FACE)
    spare_west = perms[2 * CELLS:3 * CELLS].reshape(LAT_ROWS, LAT_COLS, FACE)
    spare_south = perms[3 * CELLS:].reshape(LAT_ROWS, LAT_COLS, FACE)
    across_back = jnp.argsort(across, axis=-1, stable=True).astype(jnp.int32)
    upward_back = jnp.argsort(upward, axis=-1, stable=True).astype(jnp.int32)
    west = jnp.concatenate([spare_west[:, :1], across_back[:, :-1]], axis=1)
    south = jnp.concatenate([spare_south[:1], upward_back[:-1]], axis=0)
    stacked = jnp.stack([west, across, south, upward], axis=2)
    return stacked.reshape(CELLS, 4, FACE).astype(jnp.int32)


def touch_ends(entries, rng, smallest, top_value):
    longest = entries.shape.index(max(entries.shape))
    spots = []
    for shift in (0, 1):
        where = [jax.random.randint(jax.random.fold_in(rng, axis), (), 0, length) for axis, length in enumerate(entries.shape)]
        where[longest] = (where[longest] + shift) % entries.shape[longest]
        spots.append(tuple(where))
    return entries.at[spots[0]].set(smallest).at[spots[1]].set(top_value)


def levels(rng, dims, shards, smallest, top_value):
    def one(dim, blocks):
        heights = jax.random.uniform(jax.random.fold_in(jax.random.fold_in(rng, 6), dim), (blocks,), jnp.float32, smallest / len(shards), top_value / len(shards))
        return jnp.repeat(jnp.exp(heights), dims[dim] // blocks).reshape((-1,) + (1,) * (len(dims) - dim - 1))

    factor_of = one(*shards[0])
    for cut in shards[1:]:
        factor_of = factor_of * one(*cut)
    return factor_of


def normal_values(key, shape, scale, bound, shards=(), held_as=jnp.bfloat16):
    values = scale * jax.random.normal(key, shape, jnp.float32)
    if shards:
        values = values * levels(key, shape, shards, -0.22, 0.18)
    return jnp.clip(values, -bound, bound).astype(held_as)


def setup_inputs(seed: int = 0) -> dict:
    splits = jax.random.split(jax.random.key(seed), 10)
    return {
        "load": normal_values(splits[0], (CELLS, IFACE, RHS), 1.0, 6.0, ((0, 128),), jnp.float32),
        "schur": draw_schur(jax.random.fold_in(splits[9], 71), 0),
        "local_inverse": draw_local_inverse(jax.random.fold_in(splits[9], 71), 0),
        "face_map": draw_face_map(jax.random.fold_in(splits[9], 71), 0),
        "primal_basis": normal_values(splits[4], (CELLS, PRIM, IFACE), (IFACE // 4) ** -0.5, 0.25, ((0, 128),)),
        "primal_index": touch_ends(jax.random.randint(splits[5], (CELLS, PRIM), 0, NCG), jax.random.fold_in(splits[5], 1), 0, NCG - 1).astype(jnp.int32),
        "group_inverse": draw_group_inverse(jax.random.fold_in(splits[9], 71), 0),
        "group_to_coarsest": normal_values(splits[7], (LAT_ROWS, NCG, NQ), NCG ** -0.5, 0.1875, ((0, 4), (1, 32)), jnp.float32),
        "coarsest_inverse": draw_coarsest_inverse(jax.random.fold_in(splits[9], 71), 0),
    }


HIGHEST = lax.Precision.HIGHEST


def face_weights():
    rows = jnp.arange(LAT_ROWS)[:, None] + jnp.zeros((1, LAT_COLS), jnp.int32)
    cols = jnp.arange(LAT_COLS)[None, :] + jnp.zeros((LAT_ROWS, 1), jnp.int32)
    exists = jnp.stack([cols > 0, cols < LAT_COLS - 1, rows > 0, rows < LAT_ROWS - 1], axis=2)
    per_face = jnp.where(exists, 0.5, 1.0).astype(jnp.float32)
    return jnp.repeat(per_face, FACE, axis=2).reshape(CELLS, IFACE, 1)


def assemble(values, face_map):
    faces = values.reshape(LAT_ROWS, LAT_COLS, 4, FACE, RHS)
    zero_col = jnp.zeros((LAT_ROWS, 1, FACE, RHS), values.dtype)
    zero_row = jnp.zeros((1, LAT_COLS, FACE, RHS), values.dtype)
    from_west = jnp.concatenate([zero_col, faces[:, :-1, 1]], axis=1)
    from_east = jnp.concatenate([faces[:, 1:, 0], zero_col], axis=1)
    from_south = jnp.concatenate([zero_row, faces[:-1, :, 3]], axis=0)
    from_north = jnp.concatenate([faces[1:, :, 2], zero_row], axis=0)
    received = jnp.stack([from_west, from_east, from_south, from_north], axis=2).reshape(CELLS * 4, FACE, RHS)
    moved = jax.vmap(lambda block, order: block[order])(received, face_map.reshape(CELLS * 4, FACE))
    return values + moved.reshape(CELLS, IFACE, RHS)


def precondition(residual, weight_rows, local_inverse, face_map, primal_basis, primal_index, group_inverse, group_to_coarsest, coarsest_inverse):
    weighted = (residual * weight_rows).astype(jnp.bfloat16)

    def per_cell(items):
        matrix, basis, vector = items
        return (jnp.dot(matrix, vector, preferred_element_type=jnp.float32),
                jnp.dot(basis, vector, preferred_element_type=jnp.float32))

    local_part, primal = lax.map(per_cell, (local_inverse, primal_basis, weighted))
    owners = (jnp.arange(CELLS) // LAT_COLS)[:, None].astype(jnp.int32) * NCG + primal_index.astype(jnp.int32)
    group_coarse = jax.ops.segment_sum(primal.reshape(CELLS * PRIM, RHS), owners.reshape(-1), num_segments=LAT_ROWS * NCG)
    group_coarse = group_coarse.reshape(LAT_ROWS, NCG, RHS)
    coarsest = jnp.einsum('gkq,gkr->qr', group_to_coarsest, group_coarse, precision=HIGHEST)
    coarsest_solution = jnp.dot(coarsest_inverse, coarsest, precision=HIGHEST)
    group_solution = jnp.einsum('gkl,glr->gkr', group_inverse, group_coarse, precision=HIGHEST)
    group_solution = group_solution + jnp.einsum('gkq,qr->gkr', group_to_coarsest, coarsest_solution, precision=HIGHEST)
    picked = group_solution.reshape(LAT_ROWS * NCG, RHS)[owners]
    coarse_part = jnp.einsum('cpi,cpr->cir', primal_basis.astype(jnp.float32), picked, precision=HIGHEST)
    return assemble((local_part + coarse_part) * weight_rows, face_map)


def reference(load, schur, local_inverse, face_map, primal_basis, primal_index, group_inverse, group_to_coarsest, coarsest_inverse):
    weight_rows = face_weights()

    def apply_pre(values):
        return precondition(values, weight_rows, local_inverse, face_map, primal_basis, primal_index, group_inverse, group_to_coarsest, coarsest_inverse)

    rhs_side = assemble(load, face_map)
    solution = jnp.zeros_like(rhs_side)
    residual = rhs_side
    search = apply_pre(residual)
    direction = search
    product = jnp.sum(weight_rows * residual * search, axis=(0, 1))
    for iteration in range(ITERS):
        image_local = lax.map(lambda items: jnp.dot(items[0], items[1].astype(jnp.bfloat16), preferred_element_type=jnp.float32), (schur, direction))
        image = assemble(image_local, face_map)
        curvature = jnp.sum(weight_rows * direction * image, axis=(0, 1))
        alpha = product / curvature
        solution = solution + alpha * direction
        residual = residual - alpha * image
        if iteration + 1 < ITERS:
            search = apply_pre(residual)
            product_next = jnp.sum(weight_rows * residual * search, axis=(0, 1))
            direction = search + (product_next / product) * direction
            product = product_next
    return solution, residual
```

```python
import jax
import jax.numpy as jnp
from jax import lax
from jax.experimental import pallas as pl
from jax.experimental.pallas import tpu as pltpu
from jax.sharding import PartitionSpec as P

MESH = pl.DeviceIdType.MESH
HIGHEST = lax.Precision.HIGHEST
F32 = jnp.float32
BF16 = jnp.bfloat16

ROWS = 4
COLS = 32
IFACE = 2048
FACE = 512
RHS = 256
PRIM = 32
NQ = 128
NCG = 1024
ITERS = 2
BLOCK = NCG // COLS


def dot(a, b):
    return jnp.dot(a, b, preferred_element_type=F32)


def halves(value):
    high = value.astype(BF16)
    return high, (value - high.astype(F32)).astype(BF16)


def column_sums(value):
    return jnp.sum(value, axis=0, keepdims=True)


def eighths(value):
    return jnp.sum(value.reshape(FACE // 8, 8, RHS), axis=0)


def kernel(
    load_h, schur_h, linv_h, fmap, basis, index, ginv, lifting, cinv,
    x_out, r_out,
    sv, lv, r, t, q, zz, wb, perm, send, recv, cmat, nbsend, nbrecv,
    mysetup, srecv, gin, et, fm, whi, wlo, grc, gc,
    pbuf, xrecv, zcs, zcr, obuf, orecv, pk, pkr, red, redr, redz, redzr, acc, scal,
    load_sem, mat_sem, face_ssem, face_rsem, nb_ssem, nb_rsem, set_sem, gin_sem,
    x_sem, zc_sem, o_sem, pk_ssem, pk_rsem, red_sem, redz_sem, out_sem,
):
    g = lax.axis_index("grp")
    c = lax.axis_index("cell")
    xq = c // 8
    rest = c % 8

    def rows(f):
        return pl.ds(pl.multiple_of(f * FACE, FACE), FACE)

    def where_is(f):
        axis = f // 2
        sign = 2 * (f % 2) - 1
        gg = g + axis * sign
        cc = c + (1 - axis) * sign
        exists = jnp.logical_and(
            jnp.logical_and(gg >= 0, gg < ROWS), jnp.logical_and(cc >= 0, cc < COLS)
        )
        return exists, (gg, cc)

    def weight(f):
        exists, _ = where_is(f)
        return jnp.where(exists, 0.5, 1.0).astype(F32)

    def other(f):
        return f + 1 - 2 * (f % 2)

    load_copies = [
        pltpu.make_async_copy(
            load_h.at[pl.ds(f * FACE, FACE)], r.at[pl.ds(f * FACE, FACE)], load_sem.at[f]
        )
        for f in range(4)
    ]
    for f in (3, 2, 1, 0):
        load_copies[f].start()
    linv_copy = pltpu.make_async_copy(linv_h, lv, mat_sem.at[0])
    linv_copy.start()
    schur_copy = pltpu.make_async_copy(schur_h, sv, mat_sem.at[1])
    schur_copy.start()

    barrier = pltpu.get_barrier_semaphore()

    def greet_row(k, carry):
        pl.semaphore_signal(
            barrier, inc=1, device_id=(g, (c + k) % COLS), device_id_type=MESH
        )
        return carry

    lax.fori_loop(1, COLS, greet_row, 0)
    for k in range(1, ROWS):
        pl.semaphore_signal(
            barrier, inc=1, device_id=((g + k) % ROWS, c), device_id_type=MESH
        )

    def build_perm(f, carry):
        mine = fmap[pl.ds(f, 1), :]
        places = lax.broadcasted_iota(jnp.int32, (FACE, FACE), 0)
        perm[pl.ds(f, 1)] = jnp.where(places == mine, 1.0, 0.0).astype(BF16)[None]
        return carry

    lax.fori_loop(0, 4, build_perm, 0)
    pl.semaphore_wait(barrier, COLS - 1 + ROWS - 1)

    def face_copy(e, f):
        _, there = where_is(f)
        return pltpu.make_async_remote_copy(
            src_ref=send.at[f],
            dst_ref=recv.at[e, other(f)],
            send_sem=face_ssem.at[f],
            recv_sem=face_rsem.at[e, other(f)],
            device_id=there,
            device_id_type=MESH,
        )

    def face_arrival(e, f):
        _, there = where_is(f)
        return pltpu.make_async_remote_copy(
            src_ref=send.at[f],
            dst_ref=recv.at[e, f],
            send_sem=face_ssem.at[f],
            recv_sem=face_rsem.at[e, f],
            device_id=there,
            device_id_type=MESH,
        )

    def send_face(e, f, ref):
        exists, _ = where_is(f)

        @pl.when(exists)
        def _():
            high, low = halves(ref[rows(f)])
            order = perm[pl.ds(f, 1)].reshape(FACE, FACE)
            send[pl.ds(f, 1)] = (dot(order, high) + dot(order, low))[None]
            face_copy(e, f).start()

    def await_face(e, f):
        exists, _ = where_is(f)

        @pl.when(exists)
        def _():
            arrival = face_arrival(e, f)
            arrival.wait_recv()
            arrival.wait_send()

        @pl.when(jnp.logical_not(exists))
        def _():
            recv[pl.ds(e, 1), pl.ds(f, 1)] = jnp.zeros((1, 1, FACE, RHS), F32)

    def face_of(e, f):
        return recv[pl.ds(e, 1), pl.ds(f, 1)].reshape(FACE, RHS)

    for f in (3, 2, 1, 0):
        load_copies[f].wait()
        send_face(0, f, r)

    lane = lax.broadcasted_iota(jnp.int32, (PRIM, 128), 1)
    line = lax.broadcasted_iota(jnp.int32, (PRIM, 128), 0)
    spots = index[...].astype(F32)
    spots = jnp.broadcast_to(spots, (8, PRIM))
    low_spots = jnp.dot(
        spots, jnp.where(line == lane % 16, 1.0, 0.0).astype(F32),
        precision=HIGHEST, preferred_element_type=F32,
    )
    high_spots = jnp.dot(
        spots, jnp.where(line == lane % 16 + 16, 1.0, 0.0).astype(F32),
        precision=HIGHEST, preferred_element_type=F32,
    )
    mysetup[0:BLOCK] = lifting[...]
    mysetup[BLOCK : BLOCK + 8] = low_spots
    mysetup[BLOCK + 8 : BLOCK + 16] = high_spots
    srecv[pl.ds(c, 1)] = mysetup[...][None]

    def setup_copy(k):
        return pltpu.make_async_remote_copy(
            src_ref=mysetup,
            dst_ref=srecv.at[c],
            send_sem=set_sem.at[0],
            recv_sem=set_sem.at[1],
            device_id=(g, (c + k) % COLS),
            device_id_type=MESH,
        )

    def start_setup(k, carry):
        setup_copy(k).start()
        return carry

    lax.fori_loop(1, COLS, start_setup, 0)

    def gin_copy(k):
        return pltpu.make_async_remote_copy(
            src_ref=ginv,
            dst_ref=gin.at[xq],
            send_sem=gin_sem.at[0],
            recv_sem=gin_sem.at[1],
            device_id=(g, ((xq + k) % 4) * 8 + rest),
            device_id_type=MESH,
        )

    for k in range(1, 4):
        gin_copy(k).start()
    gin[pl.ds(xq, 1)] = ginv[...][None]

    def nb_copy(f, slot):
        _, there = where_is(f)
        return pltpu.make_async_remote_copy(
            src_ref=nbsend.at[f],
            dst_ref=nbrecv.at[slot],
            send_sem=nb_ssem.at[f],
            recv_sem=nb_rsem.at[slot],
            device_id=there,
            device_id_type=MESH,
        )

    for f in range(4):
        exists, _ = where_is(f)

        @pl.when(exists)
        def _():
            nbsend[f] = lax.dot_general(
                basis[:, f * FACE : (f + 1) * FACE], perm[f],
                (((1,), (1,)), ((), ())), preferred_element_type=F32,
            )
            nb_copy(f, f ^ 1).start()

        @pl.when(jnp.logical_not(exists))
        def _():
            nbrecv[f] = jnp.zeros((PRIM, FACE), F32)
            pkr[0, f] = jnp.zeros((PRIM, RHS), F32)
            pkr[1, f] = jnp.zeros((PRIM, RHS), F32)

    q[...] = jnp.zeros_like(q)
    scal[...] = jnp.ones_like(scal)

    def wait_bytes(ref, ssem, rsem, to):
        both = pltpu.make_async_remote_copy(
            src_ref=ref, dst_ref=ref, send_sem=ssem, recv_sem=rsem,
            device_id=to, device_id_type=MESH,
        )
        both.wait_recv()
        both.wait_send()

    row_peer = (g, (c + 1) % COLS)
    z_peer = ((g + 1) % ROWS, c)

    for f in range(4):
        exists, _ = where_is(f)

        @pl.when(exists)
        def _():
            both = nb_copy(f, f)
            both.wait_recv()
            both.wait_send()

        own = basis[:, f * FACE : (f + 1) * FACE].astype(F32)
        near = nbrecv[f]
        cmat[f] = (jnp.concatenate([own, own, near, near], axis=0) * weight(f)).T.astype(BF16)

    wait_bytes(srecv.at[pl.ds(0, COLS - 1)], set_sem.at[0], set_sem.at[1], row_peer)
    wait_bytes(gin.at[pl.ds(0, 3)], gin_sem.at[0], gin_sem.at[1], row_peer)

    lane1 = lax.broadcasted_iota(jnp.int32, (1, 128), 1)

    def spots_of(line_number):
        parts = []
        for quarter in range(4):
            total = jnp.zeros((1, 128), F32)
            for n in range(8 * quarter, 8 * quarter + 8):
                row = srecv[n, line_number : line_number + 1, :]
                total = total + jnp.where(lane1 // 16 == n % 8, row, 0.0)
            parts.append(total)
        return jnp.concatenate(parts, axis=1).astype(jnp.int32)

    wanted = jnp.concatenate([spots_of(BLOCK), spots_of(BLOCK + 8)], axis=1)

    for block in range(8):
        target = lax.broadcasted_iota(jnp.int32, (128, NCG), 0) + block * 128
        et[pl.ds(block * 128, 128)] = jnp.where(target == wanted, 1.0, 0.0).astype(BF16)

    own_row = lax.broadcasted_iota(jnp.int32, (128, NCG), 0)
    own_row = (own_row // BLOCK) * (8 * BLOCK) + rest * BLOCK + own_row % BLOCK
    fm[...] = jnp.where(own_row == wanted, 1.0, 0.0).astype(F32).T.astype(BF16)

    high, low = halves(gin[...].reshape(128, NCG))
    whi[0:128] = high
    wlo[0:128] = low
    all_lifting = srecv[:, 0:BLOCK, :].reshape(NCG, NQ)
    high, low = halves(all_lifting.T)
    whi[128:256] = high
    wlo[128:256] = low
    own_lifting = jnp.concatenate(
        [srecv[pl.ds(8 * k + rest, 1), 0:BLOCK, :].reshape(BLOCK, NQ) for k in range(4)], axis=0
    )
    grc[...] = jnp.dot(own_lifting, cinv[...], precision=HIGHEST, preferred_element_type=F32)

    linv_copy.wait()
    schur_copy.wait()

    def settle_start(i, carry):
        await_face(0, i)
        value = r[rows(i)] + face_of(0, i)
        r[rows(i)] = value
        wb[rows(i)] = (value * weight(i)).astype(BF16)
        return carry

    lax.fori_loop(0, 4, settle_start, 0)

    lane_wide = lax.broadcasted_iota(jnp.int32, (16, 128), 1)

    def left(shape):
        return lax.broadcasted_iota(jnp.int32, shape, 1) < 64

    def swap(value):
        return pltpu.roll(value, 64, 1)

    def coarse(it):
        def x_copy(k):
            there = (c + k) % COLS
            return pltpu.make_async_remote_copy(
                src_ref=pbuf.at[there // 8],
                dst_ref=xrecv.at[it, c],
                send_sem=x_sem.at[it, 0],
                recv_sem=x_sem.at[it, 1],
                device_id=(g, there),
                device_id_type=MESH,
            )

        primal = dot(basis[...], wb[...])
        for pair in range(2):
            part = primal[:, 128 * pair : 128 * pair + 128]
            top, bottom = part[0:16], part[16:32]
            pbuf[2 * pair] = jnp.where(lane_wide < 64, top, swap(bottom))
            pbuf[2 * pair + 1] = jnp.where(lane_wide < 64, swap(top), bottom)

        def start(k, carry):
            x_copy(k).start()
            return carry

        lax.fori_loop(1, COLS, start, 0)
        xrecv[pl.ds(it, 1), pl.ds(c, 1)] = pbuf[pl.ds(xq, 1)][None]

    def solve_coarse(it):
        wait_bytes(xrecv.at[it, pl.ds(0, COLS - 1)], x_sem.at[it, 0], x_sem.at[it, 1], row_peer)
        block = xrecv[pl.ds(it, 1)].reshape(FACE, 128)
        parts = jnp.concatenate(halves(block), axis=1)
        upper = dot(et[:, 0:512], parts)
        lower = dot(et[:, 512:1024], parts)
        upper = upper[:, 0:128] + upper[:, 128:256]
        lower = lower[:, 0:128] + lower[:, 128:256]
        gc[...] = upper + swap(lower)
        high, low = halves(gc[...])
        both = dot(whi[...], jnp.concatenate([high, low], axis=1))
        both = both[:, 0:128] + both[:, 128:256] + dot(wlo[...], high)
        from_row = both[0:128]
        partial = both[128:256]
        packed = jnp.where(left((64, 128)), partial[0:64], swap(partial[64:128]))
        zcs[...] = packed
        zcr[pl.ds(it, 1), pl.ds(g, 1)] = packed[None, None]

        def z_copy(k):
            return pltpu.make_async_remote_copy(
                src_ref=zcs,
                dst_ref=zcr.at[it, g],
                send_sem=zc_sem.at[it, 0],
                recv_sem=zc_sem.at[it, 1],
                device_id=((g + k) % ROWS, c),
                device_id_type=MESH,
            )

        for k in range(1, ROWS):
            z_copy(k).start()
        wait_bytes(zcr.at[it, pl.ds(0, ROWS - 1)], zc_sem.at[it, 0], zc_sem.at[it, 1], z_peer)
        blocks = zcr[pl.ds(it, 1)].reshape(ROWS, 64, 128)
        total = (blocks[0] + blocks[1]) + (blocks[2] + blocks[3])
        coarsest = jnp.concatenate([total, swap(total)], axis=0)
        owned = from_row + jnp.dot(
            grc[...], coarsest, precision=HIGHEST, preferred_element_type=F32
        )
        parts = jnp.concatenate(halves(owned), axis=1)
        back = dot(fm[...], parts)
        back = back[:, 0:128] + back[:, 128:256]
        packed = jnp.where(left((FACE, 128)), back[0:512], swap(back[512:1024]))
        obuf[...] = packed.reshape(COLS, 16, 128)

        def o_copy(k):
            there = (c + k) % COLS
            return pltpu.make_async_remote_copy(
                src_ref=obuf.at[there],
                dst_ref=orecv.at[it, c],
                send_sem=o_sem.at[it, 0],
                recv_sem=o_sem.at[it, 1],
                device_id=(g, there),
                device_id_type=MESH,
            )

        def start(k, carry):
            o_copy(k).start()
            return carry

        lax.fori_loop(1, COLS, start, 0)
        orecv[pl.ds(it, 1), pl.ds(c, 1)] = obuf[pl.ds(c, 1)][None]
        wait_bytes(orecv.at[it, pl.ds(0, COLS - 1)], o_sem.at[it, 0], o_sem.at[it, 1], row_peer)
        arrived = orecv[pl.ds(it, 1)].reshape(4, 8, 16, 128)
        sums = jnp.sum(arrived, axis=1)
        columns = []
        for pair in range(2):
            first, second = sums[2 * pair], sums[2 * pair + 1]
            top = jnp.where(lane_wide < 64, first, swap(second))
            bottom = jnp.where(lane_wide < 64, swap(first), second)
            columns.append(jnp.concatenate([top, bottom], axis=0))
        pk[...] = jnp.concatenate(columns, axis=1)

        def pk_copy(f, slot):
            _, there = where_is(f)
            return pltpu.make_async_remote_copy(
                src_ref=pk,
                dst_ref=pkr.at[it, slot],
                send_sem=pk_ssem.at[f],
                recv_sem=pk_rsem.at[it, slot],
                device_id=there,
                device_id_type=MESH,
            )

        for f in range(4):
            exists, _ = where_is(f)

            @pl.when(exists)
            def _():
                pk_copy(f, f ^ 1).start()

        for f in range(4):
            exists, _ = where_is(f)

            @pl.when(exists)
            def _():
                arrival = pk_copy(f, f)
                arrival.wait_recv()
                arrival.wait_send()

    def step(it, carry):
        acc[...] = jnp.zeros_like(acc)
        first = 1 + 2 * it
        second = 2 + 2 * it

        coarse(it)

        def local(i, carry):
            f = 3 - i
            t[rows(f)] = dot(lv[rows(f)], wb[...]) * weight(f)
            send_face(first, f, t)
            return carry

        lax.fori_loop(0, 4, local, 0)
        solve_coarse(it)
        own_high, own_low = halves(pk[...])

        def settle(f, carry):
            await_face(first, f)
            near_high, near_low = halves(
                pkr[pl.ds(it, 1), pl.ds(f, 1)].reshape(PRIM, RHS)
            )
            stack = jnp.concatenate([own_high, own_low, near_high, near_low], axis=0)
            rank = dot(cmat[pl.ds(f, 1)].reshape(FACE, 128), stack)
            value = t[rows(f)] + face_of(first, f) + rank
            zz[pl.ds(it, 1), rows(f)] = value[None]
            wide = weight(f)
            acc[0] += wide * eighths(value * r[rows(f)])
            acc[1] += wide * eighths(value * q[rows(f)])
            return carry

        lax.fori_loop(0, 4, settle, 0)

        def narrow(f, carry):
            wb[rows(f)] = zz[pl.ds(it, 1), rows(f)].reshape(FACE, RHS).astype(BF16)
            return carry

        lax.fori_loop(0, 4, narrow, 0)

        def stiff(i, carry):
            f = 3 - i
            value = dot(sv[rows(f)], wb[...])
            t[rows(f)] = value
            send_face(second, f, t)
            acc[2] += eighths(value * zz[pl.ds(it, 1), rows(f)].reshape(FACE, RHS))
            acc[3] += eighths(value * zz[0, rows(f)])
            return carry

        lax.fori_loop(0, 4, stiff, 0)
        red[...] = jnp.zeros_like(red)
        for k in range(4):
            red[k : k + 1] = column_sums(acc[k])

        def red_copy(k):
            return pltpu.make_async_remote_copy(
                src_ref=red,
                dst_ref=redr.at[it, c],
                send_sem=red_sem.at[it, 0],
                recv_sem=red_sem.at[it, 1],
                device_id=(g, (c + k) % COLS),
                device_id_type=MESH,
            )

        def start(k, carry):
            red_copy(k).start()
            return carry

        lax.fori_loop(1, COLS, start, 0)
        redr[pl.ds(it, 1), pl.ds(c, 1)] = red[...][None, None]
        wait_bytes(
            redr.at[it, pl.ds(0, COLS - 1)], red_sem.at[it, 0], red_sem.at[it, 1], row_peer
        )
        row_sum = jnp.sum(redr[pl.ds(it, 1)].reshape(COLS, 8, RHS), axis=0)
        redz[...] = row_sum
        redzr[pl.ds(it, 1), pl.ds(g, 1)] = row_sum[None, None]

        def redz_copy(k):
            return pltpu.make_async_remote_copy(
                src_ref=redz,
                dst_ref=redzr.at[it, g],
                send_sem=redz_sem.at[it, 0],
                recv_sem=redz_sem.at[it, 1],
                device_id=((g + k) % ROWS, c),
                device_id_type=MESH,
            )

        for k in range(1, ROWS):
            redz_copy(k).start()
        wait_bytes(
            redzr.at[it, pl.ds(0, ROWS - 1)], redz_sem.at[it, 0], redz_sem.at[it, 1], z_peer
        )
        sums = jnp.sum(redzr[pl.ds(it, 1)].reshape(ROWS, 8, RHS), axis=0)
        rz = sums[0:1]
        beta = jnp.where(it > 0, rz / scal[0:1], 0.0)
        curv = sums[2:3] + beta * (sums[1:2] + sums[3:4]) + beta * beta * scal[1:2]
        alpha = rz / curv
        scal[3:4] = scal[2:3]
        scal[0:1] = rz
        scal[1:2] = curv
        scal[2:3] = alpha
        scal[4:5] = beta

        def update(f, carry):
            await_face(second, f)
            image = t[rows(f)] + face_of(second, f) + beta * q[rows(f)]
            q[rows(f)] = image
            value = r[rows(f)] - alpha * image
            r[rows(f)] = value
            wb[rows(f)] = (value * weight(f)).astype(BF16)
            return carry

        lax.fori_loop(0, 4, update, 0)
        return carry

    lax.fori_loop(0, ITERS, step, 0)
    alpha = scal[2:3]
    held = scal[3:4] + alpha * scal[4:5]

    def finish(f, carry):
        t[rows(f)] = held * zz[0, rows(f)] + alpha * zz[1, rows(f)]
        return carry

    r_copy = pltpu.make_async_copy(r, r_out, out_sem.at[0])
    r_copy.start()
    lax.fori_loop(0, 4, finish, 0)
    x_copy = pltpu.make_async_copy(t, x_out, out_sem.at[1])
    x_copy.start()
    r_copy.wait()
    x_copy.wait()


def body(
    load, schur, local_inverse, face_map, primal_basis, primal_index,
    group_inverse, group_to_coarsest, coarsest_inverse,
):
    anywhere = pl.BlockSpec(memory_space=pl.ANY)
    near = pl.BlockSpec(memory_space=pltpu.VMEM)
    dma = pltpu.SemaphoreType.DMA
    out = jax.ShapeDtypeStruct((IFACE, RHS), F32)
    x, r = pl.pallas_call(
        kernel,
        out_shape=(out, out),
        in_specs=[anywhere] * 3 + [near] * 6,
        out_specs=(anywhere, anywhere),
        scratch_shapes=[
            pltpu.VMEM((IFACE, IFACE), BF16),
            pltpu.VMEM((IFACE, IFACE), BF16),
            pltpu.VMEM((IFACE, RHS), F32),
            pltpu.VMEM((IFACE, RHS), F32),
            pltpu.VMEM((IFACE, RHS), F32),
            pltpu.VMEM((ITERS, IFACE, RHS), F32),
            pltpu.VMEM((IFACE, RHS), BF16),
            pltpu.VMEM((4, FACE, FACE), BF16),
            pltpu.VMEM((4, FACE, RHS), F32),
            pltpu.VMEM((1 + 2 * ITERS, 4, FACE, RHS), F32),
            pltpu.VMEM((4, FACE, 128), BF16),
            pltpu.VMEM((4, PRIM, FACE), F32),
            pltpu.VMEM((4, PRIM, FACE), F32),
            pltpu.VMEM((BLOCK + 16, NQ), F32),
            pltpu.VMEM((COLS, BLOCK + 16, NQ), F32),
            pltpu.VMEM((4, BLOCK, NCG), F32),
            pltpu.VMEM((NCG, NCG), BF16),
            pltpu.VMEM((NCG, 128), BF16),
            pltpu.VMEM((256, NCG), BF16),
            pltpu.VMEM((256, NCG), BF16),
            pltpu.VMEM((128, NQ), F32),
            pltpu.VMEM((NCG, 128), F32),
            pltpu.VMEM((4, 16, 128), F32),
            pltpu.VMEM((ITERS, COLS, 16, 128), F32),
            pltpu.VMEM((64, 128), F32),
            pltpu.VMEM((ITERS, ROWS, 64, 128), F32),
            pltpu.VMEM((COLS, 16, 128), F32),
            pltpu.VMEM((ITERS, COLS, 16, 128), F32),
            pltpu.VMEM((PRIM, RHS), F32),
            pltpu.VMEM((ITERS, 4, PRIM, RHS), F32),
            pltpu.VMEM((8, RHS), F32),
            pltpu.VMEM((ITERS, COLS, 8, RHS), F32),
            pltpu.VMEM((8, RHS), F32),
            pltpu.VMEM((ITERS, ROWS, 8, RHS), F32),
            pltpu.VMEM((4, 8, RHS), F32),
            pltpu.VMEM((8, RHS), F32),
            dma((4,)), dma((2,)), dma((4,)), dma((1 + 2 * ITERS, 4)),
            dma((4,)), dma((4,)), dma((2,)), dma((2,)),
            dma((ITERS, 2)), dma((ITERS, 2)), dma((ITERS, 2)),
            dma((4,)), dma((ITERS, 4)), dma((ITERS, 2)), dma((ITERS, 2)), dma((2,)),
        ],
        compiler_params=pltpu.CompilerParams(
            collective_id=0, has_side_effects=True, vmem_limit_bytes=63 * 1024 * 1024
        ),
    )(
        load[0], schur[0], local_inverse[0], face_map[0], primal_basis[0], primal_index,
        group_inverse[0], group_to_coarsest[0], coarsest_inverse,
    )
    return x[None], r[None]


def solution(mesh):
    spread = ("grp", "cell")
    in_specs = (
        P(spread, None, None),
        P(spread, None, None),
        P(spread, None, None),
        P(spread, None, None),
        P(spread, None, None),
        P(spread, None),
        P("grp", "cell", None),
        P("grp", "cell", None),
        P(),
    )
    out_specs = (P(spread, None, None), P(spread, None, None))
    return jax.shard_map(body, mesh=mesh, in_specs=in_specs, out_specs=out_specs, check_vma=False)
```

```python
import jax
import jax.numpy as jnp
from jax import lax
from jax.experimental import pallas as pl
from jax.experimental.pallas import tpu as pltpu
from jax.sharding import PartitionSpec as P

MESH = pl.DeviceIdType.MESH
HIGHEST = lax.Precision.HIGHEST
F32 = jnp.float32
BF16 = jnp.bfloat16

ROWS = 4
COLS = 32
IFACE = 2048
FACE = 512
RHS = 256
PRIM = 32
NQ = 128
NCG = 1024
ITERS = 2
BLOCK = NCG // COLS
CUT_LOCAL = 384
CUT_AGAIN = 128
CUT_STIFF = 128
CUT_SIDE = 256


def dot(a, b):
    return jnp.dot(a, b, preferred_element_type=F32)


def halves(value):
    high = value.astype(BF16)
    return high, (value - high.astype(F32)).astype(BF16)


def column_sums(value):
    return jnp.sum(value, axis=0, keepdims=True)


def eighths(value):
    return jnp.sum(value.reshape(FACE // 8, 8, RHS), axis=0)


def kernel(
    load_h, schur_h, linv_h, fmap, basis, index, ginv, lifting, cinv,
    x_out, r_out,
    sv, lv, r, t, q, zz, wb, perm, send, recv, cmat, nbsend, nbrecv,
    myspots, prow, srecv, gin, et, fm, whi, wlo, egc, gc, chat, sc, css, csr, pkhl,
    pbuf, xrecv, zcs, zcr, obuf, orecv, pk, pkr, red, redr, redz, redzr, acc, scal,
    pmat, ems, emr, pq, pkb,
    load_sem, mat_sem, face_ssem, face_rsem, nb_ssem, nb_rsem, spot_sem, set_sem, gin_sem,
    x_sem, zc_sem, cs_sem, o_sem, pk_ssem, pk_rsem, red_sem, redz_sem, out_sem, em_ssem, em_rsem,
):
    g = lax.axis_index("grp")
    c = lax.axis_index("cell")
    xq = c // 8
    rest = c % 8

    def rows(f):
        return pl.ds(pl.multiple_of(f * FACE, FACE), FACE)

    def where_is(f):
        axis = f // 2
        sign = 2 * (f % 2) - 1
        gg = g + axis * sign
        cc = c + (1 - axis) * sign
        exists = jnp.logical_and(
            jnp.logical_and(gg >= 0, gg < ROWS), jnp.logical_and(cc >= 0, cc < COLS)
        )
        return exists, (gg, cc)

    def weight(f):
        exists, _ = where_is(f)
        return jnp.where(exists, 0.5, 1.0).astype(F32)

    def other(f):
        return f + 1 - 2 * (f % 2)

    load_copies = [
        pltpu.make_async_copy(
            load_h.at[pl.ds(f * FACE, FACE)], r.at[pl.ds(f * FACE, FACE)], load_sem.at[f]
        )
        for f in range(4)
    ]
    for f in (3, 2, 1, 0):
        load_copies[f].start()
    linv_copy = pltpu.make_async_copy(linv_h, lv, mat_sem.at[0])
    schur_copy = pltpu.make_async_copy(schur_h, sv, mat_sem.at[1])

    barrier = pltpu.get_barrier_semaphore()

    def greet_row(k, carry):
        pl.semaphore_signal(
            barrier, inc=1, device_id=(g, (c + k) % COLS), device_id_type=MESH
        )
        return carry

    lax.fori_loop(1, COLS, greet_row, 0)
    for k in range(1, ROWS):
        pl.semaphore_signal(
            barrier, inc=1, device_id=((g + k) % ROWS, c), device_id_type=MESH
        )

    def build_perm(f, carry):
        mine = fmap[pl.ds(f, 1), :]
        places = lax.broadcasted_iota(jnp.int32, (FACE, FACE), 0)
        perm[pl.ds(f, 1)] = jnp.where(places == mine, 1.0, 0.0).astype(BF16)[None]
        return carry

    lax.fori_loop(0, 4, build_perm, 0)

    def face_copy(e, f, start, stop):
        _, there = where_is(f)
        return pltpu.make_async_remote_copy(
            src_ref=send.at[f, pl.ds(start, stop - start)],
            dst_ref=recv.at[e, other(f), pl.ds(start, stop - start)],
            send_sem=face_ssem.at[f],
            recv_sem=face_rsem.at[e, other(f)],
            device_id=there,
            device_id_type=MESH,
        )

    def face_arrival(e, f):
        _, there = where_is(f)
        return pltpu.make_async_remote_copy(
            src_ref=send.at[f],
            dst_ref=recv.at[e, f],
            send_sem=face_ssem.at[f],
            recv_sem=face_rsem.at[e, f],
            device_id=there,
            device_id_type=MESH,
        )

    def order_face(f, ref):
        exists, _ = where_is(f)

        @pl.when(exists)
        def _():
            high, low = halves(ref[rows(f)])
            order = perm[pl.ds(f, 1)].reshape(FACE, FACE)
            send[pl.ds(f, 1)] = (dot(order, high) + dot(order, low))[None]

    def start_face(e, f, start, stop):
        exists, _ = where_is(f)

        @pl.when(exists)
        def _():
            face_copy(e, f, start, stop).start()

    def await_face(e, f):
        exists, _ = where_is(f)

        @pl.when(exists)
        def _():
            arrival = face_arrival(e, f)
            arrival.wait_recv()
            arrival.wait_send()

        @pl.when(jnp.logical_not(exists))
        def _():
            recv[pl.ds(e, 1), pl.ds(f, 1)] = jnp.zeros((1, 1, FACE, RHS), F32)

    def face_of(e, f):
        return recv[pl.ds(e, 1), pl.ds(f, 1)].reshape(FACE, RHS)

    for f in (3, 2, 1, 0):
        load_copies[f].wait()
        if f == 3:
            linv_copy.start()
            schur_copy.start()
        order_face(f, r)

    lane = lax.broadcasted_iota(jnp.int32, (PRIM, 128), 1)
    line = lax.broadcasted_iota(jnp.int32, (PRIM, 128), 0)
    spots = jnp.broadcast_to(index[...].astype(F32), (8, PRIM))
    low_spots = jnp.dot(
        spots, jnp.where(line == lane % 16, 1.0, 0.0).astype(F32),
        precision=HIGHEST, preferred_element_type=F32,
    )
    high_spots = jnp.dot(
        spots, jnp.where(line == lane % 16 + 16, 1.0, 0.0).astype(F32),
        precision=HIGHEST, preferred_element_type=F32,
    )
    first_line = lax.broadcasted_iota(jnp.int32, (8, 128), 0) == 0
    myspots[...] = jnp.where(first_line, low_spots, high_spots)
    prow[pl.ds(c, 1)] = myspots[...][None]
    srecv[pl.ds(c, 1)] = lifting[...][None]
    gin[pl.ds(xq, 1)] = ginv[...][None]

    pl.semaphore_wait(barrier, COLS - 1 + ROWS - 1)
    start_face(0, 3, 0, FACE)
    start_face(0, 2, 0, FACE)

    def spots_copy(k):
        return pltpu.make_async_remote_copy(
            src_ref=myspots,
            dst_ref=prow.at[c],
            send_sem=spot_sem.at[0],
            recv_sem=spot_sem.at[1],
            device_id=(g, (c + k) % COLS),
            device_id_type=MESH,
        )

    def start_spots(k, carry):
        spots_copy(k).start()
        return carry

    lax.fori_loop(1, COLS, start_spots, 0)
    start_face(0, 1, 0, FACE)
    start_face(0, 0, 0, FACE)

    def setup_copy(k):
        return pltpu.make_async_remote_copy(
            src_ref=lifting,
            dst_ref=srecv.at[c],
            send_sem=set_sem.at[0],
            recv_sem=set_sem.at[1],
            device_id=(g, (c + k) % COLS),
            device_id_type=MESH,
        )

    def start_setup(k, carry):
        setup_copy(k).start()
        return carry

    def gin_copy(k):
        return pltpu.make_async_remote_copy(
            src_ref=ginv,
            dst_ref=gin.at[xq],
            send_sem=gin_sem.at[0],
            recv_sem=gin_sem.at[1],
            device_id=(g, ((xq + k) % 4) * 8 + rest),
            device_id_type=MESH,
        )

    for k in range(1, 4):
        gin_copy(k).start()
    lax.fori_loop(1, COLS, start_setup, 0)

    def nb_copy(f, slot):
        _, there = where_is(f)
        return pltpu.make_async_remote_copy(
            src_ref=nbsend.at[f],
            dst_ref=nbrecv.at[slot],
            send_sem=nb_ssem.at[f],
            recv_sem=nb_rsem.at[slot],
            device_id=there,
            device_id_type=MESH,
        )

    for f in range(4):
        exists, _ = where_is(f)

        @pl.when(exists)
        def _():
            nbsend[f] = lax.dot_general(
                basis[:, f * FACE : (f + 1) * FACE], perm[f],
                (((1,), (1,)), ((), ())), preferred_element_type=F32,
            )
            nb_copy(f, f ^ 1).start()

        @pl.when(jnp.logical_not(exists))
        def _():
            nbrecv[f] = jnp.zeros((PRIM, FACE), F32)
            pkr[0, f] = jnp.zeros((PRIM, RHS), F32)
            pkr[1, f] = jnp.zeros((PRIM, RHS), F32)
            emr[f] = jnp.zeros((PRIM, RHS), F32)

    q[...] = jnp.zeros_like(q)
    scal[...] = jnp.ones_like(scal)

    def wait_bytes(ref, ssem, rsem, to):
        both = pltpu.make_async_remote_copy(
            src_ref=ref, dst_ref=ref, send_sem=ssem, recv_sem=rsem,
            device_id=to, device_id_type=MESH,
        )
        both.wait_recv()
        both.wait_send()

    row_peer = (g, (c + 1) % COLS)
    z_peer = ((g + 1) % ROWS, c)

    wait_bytes(prow.at[pl.ds(0, COLS - 1)], spot_sem.at[0], spot_sem.at[1], row_peer)

    lane1 = lax.broadcasted_iota(jnp.int32, (1, 128), 1)

    def spots_of(line_number):
        parts = []
        for quarter in range(4):
            total = jnp.zeros((1, 128), F32)
            for n in range(8 * quarter, 8 * quarter + 8):
                row = prow[n, line_number : line_number + 1, :]
                total = total + jnp.where(lane1 // 16 == n % 8, row, 0.0)
            parts.append(total)
        return jnp.concatenate(parts, axis=1).astype(jnp.int32)

    wanted = jnp.concatenate([spots_of(0), spots_of(1)], axis=1)

    for block in range(8):
        target = lax.broadcasted_iota(jnp.int32, (128, NCG), 0) + block * 128
        et[pl.ds(block * 128, 128)] = jnp.where(target == wanted, 1.0, 0.0).astype(BF16)

    own_row = lax.broadcasted_iota(jnp.int32, (128, NCG), 0)
    own_row = (own_row // BLOCK) * (8 * BLOCK) + rest * BLOCK + own_row % BLOCK
    fm[...] = jnp.where(own_row == wanted, 1.0, 0.0).astype(F32).T.astype(BF16)

    wait_bytes(gin.at[pl.ds(0, 3)], gin_sem.at[0], gin_sem.at[1], row_peer)
    high, low = halves(gin[...].reshape(128, NCG))
    whi[0:128] = high
    wlo[0:128] = low

    def build_late():
        wait_bytes(srecv.at[pl.ds(0, COLS - 1)], set_sem.at[0], set_sem.at[1], row_peer)
        all_lifting = srecv[...].reshape(NCG, NQ)
        high, low = halves(all_lifting.T)
        whi[128:256] = high
        wlo[128:256] = low
        mine = jnp.where(lane1 < 16, myspots[0:1], myspots[1:2]).astype(jnp.int32)
        target = lax.broadcasted_iota(jnp.int32, (NCG, 128), 0)
        chosen = jnp.where(target == mine, 1.0, 0.0).astype(F32).T[0:PRIM].astype(BF16)
        high, low = halves(all_lifting)
        egc[...] = jnp.dot(
            dot(chosen, high) + dot(chosen, low), cinv[...],
            precision=HIGHEST, preferred_element_type=F32,
        )

    def build_rank():
        for f in range(4):
            exists, _ = where_is(f)

            @pl.when(exists)
            def _():
                both = nb_copy(f, f)
                both.wait_recv()
                both.wait_send()

            own = basis[:, f * FACE : (f + 1) * FACE].astype(F32)
            near = nbrecv[f]
            stack = jnp.concatenate([own, own, near, near], axis=0) * weight(f)
            cmat[f] = stack.T.astype(BF16)
            pmat[f] = (jnp.concatenate([own, near], axis=0) * weight(f)).astype(BF16)
            empty = jnp.zeros((PRIM, FACE), F32)
            stack = jnp.concatenate(
                [own] + [near if k == f else empty for k in range(4)] + [empty] * 3, axis=0
            )
            chat[f * FACE : (f + 1) * FACE] = (stack * weight(f)).T.astype(BF16)

        def build_images(f, carry):
            high, low = halves(dot(sv[rows(f)], chat[...]))
            sc[rows(f), 0:256] = high
            sc[rows(f), 256:512] = low
            return carry

        lax.fori_loop(0, 4, build_images, 0)

    linv_copy.wait()
    schur_copy.wait()

    def settle_start(i, carry):
        await_face(0, i)
        value = r[rows(i)] + face_of(0, i)
        r[rows(i)] = value
        wb[rows(i)] = (value * weight(i)).astype(BF16)
        return carry

    lax.fori_loop(0, 4, settle_start, 0)

    lane_wide = lax.broadcasted_iota(jnp.int32, (16, 128), 1)

    def left(shape):
        return lax.broadcasted_iota(jnp.int32, shape, 1) < 64

    def swap(value):
        return pltpu.roll(value, 64, 1)

    def coarse(it, primal):
        def x_copy(k):
            there = (c + k) % COLS
            return pltpu.make_async_remote_copy(
                src_ref=pbuf.at[there // 8],
                dst_ref=xrecv.at[it, c],
                send_sem=x_sem.at[it, 0],
                recv_sem=x_sem.at[it, 1],
                device_id=(g, there),
                device_id_type=MESH,
            )

        for pair in range(2):
            part = primal[:, 128 * pair : 128 * pair + 128]
            top, bottom = part[0:16], part[16:32]
            pbuf[2 * pair] = jnp.where(lane_wide < 64, top, swap(bottom))
            pbuf[2 * pair + 1] = jnp.where(lane_wide < 64, swap(top), bottom)

        def start(k, carry):
            x_copy(k).start()
            return carry

        lax.fori_loop(1, COLS, start, 0)
        xrecv[pl.ds(it, 1), pl.ds(c, 1)] = pbuf[pl.ds(xq, 1)][None]

    def unpack(blocks, half):
        columns = []
        lanes = left((half, 128))
        for pair in range(2):
            first, second = blocks[2 * pair], blocks[2 * pair + 1]
            top = jnp.where(lanes, first, swap(second))
            bottom = jnp.where(lanes, swap(first), second)
            columns.append(jnp.concatenate([top, bottom], axis=0))
        return jnp.concatenate(columns, axis=1)

    def solve_row(it, cut):
        wait_bytes(xrecv.at[it, pl.ds(0, COLS - 1)], x_sem.at[it, 0], x_sem.at[it, 1], row_peer)
        block = xrecv[pl.ds(it, 1)].reshape(FACE, 128)
        parts = jnp.concatenate(halves(block), axis=1)
        upper = dot(et[:, 0:512], parts)
        lower = dot(et[:, 512:1024], parts)
        upper = upper[:, 0:128] + upper[:, 128:256]
        lower = lower[:, 0:128] + lower[:, 128:256]
        gc[...] = upper + swap(lower)
        high, low = halves(gc[...])
        both = dot(whi[...], jnp.concatenate([high, low], axis=1))
        both = both[:, 0:128] + both[:, 128:256] + dot(wlo[...], high)
        partial = both[128:256]
        packed = jnp.where(left((64, 128)), partial[0:64], swap(partial[64:128]))
        zcs[...] = packed
        zcr[pl.ds(it, 1), pl.ds(g, 1)] = packed[None, None]

        def z_copy(k):
            return pltpu.make_async_remote_copy(
                src_ref=zcs,
                dst_ref=zcr.at[it, g],
                send_sem=zc_sem.at[it, 0],
                recv_sem=zc_sem.at[it, 1],
                device_id=((g + k) % ROWS, c),
                device_id_type=MESH,
            )

        for k in range(1, ROWS):
            z_copy(k).start()
        start_face(1 + 2 * it, 3, cut, FACE)
        start_face(1 + 2 * it, 2, cut, FACE)
        parts = jnp.concatenate(halves(both[0:128]), axis=1)
        back = dot(fm[...], parts)
        back = back[:, 0:128] + back[:, 128:256]
        packed = jnp.where(left((FACE, 128)), back[0:512], swap(back[512:1024]))
        obuf[...] = packed.reshape(COLS, 16, 128)

        def o_copy(k):
            there = (c + k) % COLS
            return pltpu.make_async_remote_copy(
                src_ref=obuf.at[there],
                dst_ref=orecv.at[it, c],
                send_sem=o_sem.at[it, 0],
                recv_sem=o_sem.at[it, 1],
                device_id=(g, there),
                device_id_type=MESH,
            )

        def start(k, carry):
            o_copy(k).start()
            return carry

        lax.fori_loop(1, COLS, start, 0)
        orecv[pl.ds(it, 1), pl.ds(c, 1)] = obuf[pl.ds(c, 1)][None]

    def solve_coarsest(it):
        wait_bytes(zcr.at[it, pl.ds(0, ROWS - 1)], zc_sem.at[it, 0], zc_sem.at[it, 1], z_peer)
        blocks = zcr[pl.ds(it, 1)].reshape(ROWS, 64, 128)
        total = (blocks[0] + blocks[1]) + (blocks[2] + blocks[3])
        css[...] = total
        csr[pl.ds(it, 1), pl.ds(xq, 1)] = total[None, None]

        def cs_copy(k):
            return pltpu.make_async_remote_copy(
                src_ref=css,
                dst_ref=csr.at[it, xq],
                send_sem=cs_sem.at[it, 0],
                recv_sem=cs_sem.at[it, 1],
                device_id=(g, ((xq + k) % 4) * 8 + rest),
                device_id_type=MESH,
            )

        for k in range(1, 4):
            cs_copy(k).start()

    def pk_copy(it, f, slot):
        _, there = where_is(f)
        return pltpu.make_async_remote_copy(
            src_ref=pk,
            dst_ref=pkr.at[it, slot],
            send_sem=pk_ssem.at[f],
            recv_sem=pk_rsem.at[it, slot],
            device_id=there,
            device_id_type=MESH,
        )

    def pick(it):
        wait_bytes(csr.at[it, pl.ds(0, 3)], cs_sem.at[it, 0], cs_sem.at[it, 1], row_peer)
        coarsest = unpack([csr[it, k] for k in range(4)], 64)
        wait_bytes(orecv.at[it, pl.ds(0, COLS - 1)], o_sem.at[it, 0], o_sem.at[it, 1], row_peer)
        sums = jnp.sum(orecv[pl.ds(it, 1)].reshape(4, 8, 16, 128), axis=1)
        found = unpack([sums[k] for k in range(4)], 16) + jnp.dot(
            egc[...], coarsest, precision=HIGHEST, preferred_element_type=F32
        )

        @pl.when(it == 0)
        def _():
            pk[...] = found
            pkb[...] = found

        @pl.when(it > 0)
        def _():
            pk[...] = pkb[...] - scal[2:3] * found

        for f in range(4):
            exists, _ = where_is(f)

            @pl.when(exists)
            def _():
                pk_copy(it, f, f ^ 1).start()

    def await_picks(it):
        for f in range(4):
            exists, _ = where_is(f)

            @pl.when(exists)
            def _():
                arrival = pk_copy(it, f, f)
                arrival.wait_recv()
                arrival.wait_send()

    def em_copy(f, slot):
        _, there = where_is(f)
        return pltpu.make_async_remote_copy(
            src_ref=ems.at[f],
            dst_ref=emr.at[slot],
            send_sem=em_ssem.at[f],
            recv_sem=em_rsem.at[slot],
            device_id=there,
            device_id_type=MESH,
        )

    def early_send():
        pq[...] = jnp.zeros_like(pq)

        def one(i, carry):
            f = 3 - i
            both = dot(pmat[pl.ds(f, 1)].reshape(2 * PRIM, FACE), jnp.concatenate(
                halves(t[rows(f)]), axis=1
            ))
            both = both[:, 0:RHS] + both[:, RHS:]
            pq[...] += both[0:PRIM]
            ems[pl.ds(f, 1)] = both[PRIM:][None]
            exists, _ = where_is(f)

            @pl.when(exists)
            def _():
                em_copy(f, other(f)).start()

            return carry

        lax.fori_loop(0, 4, one, 0)

    def early_launch():
        for f in range(4):
            exists, _ = where_is(f)

            @pl.when(exists)
            def _():
                arrival = em_copy(f, f)
                arrival.wait_recv()
                arrival.wait_send()

        coarse(1, pq[...] + ((emr[0] + emr[1]) + (emr[2] + emr[3])))

    def step(it, carry):
        acc[...] = jnp.zeros_like(acc)
        first = 1 + 2 * it
        second = 2 + 2 * it

        pl.when(it == 0)(lambda: coarse(0, dot(basis[...], wb[...])))

        def local(i, carry):
            f = 3 - i
            t[rows(f)] = dot(lv[rows(f)], wb[...]) * weight(f)
            order_face(f, t)

            @pl.when(jnp.logical_and(i < 2, it == 0))
            def _():
                start_face(first, f, 0, CUT_LOCAL)

            @pl.when(jnp.logical_and(i < 2, it > 0))
            def _():
                start_face(first, f, 0, CUT_AGAIN)

            @pl.when(i >= 2)
            def _():
                start_face(first, f, 0, FACE)

            return carry

        lax.fori_loop(0, 2, local, 0)
        pl.when(it > 0)(lambda: solve_row(1, CUT_AGAIN))
        lax.fori_loop(2, 4, local, 0)

        @pl.when(it == 0)
        def _():
            build_late()
            solve_row(0, CUT_LOCAL)
            build_rank()

        solve_coarsest(it)
        pl.when(it > 0)(lambda: pick(it))

        def settle(f, carry):
            await_face(first, f)
            value = t[rows(f)] + face_of(first, f)
            zz[pl.ds(it, 1), rows(f)] = value[None]
            wb[rows(f)] = value.astype(BF16)
            return carry

        lax.fori_loop(0, 4, settle, 0)

        def stiff(i, carry):
            f = 3 - i
            t[rows(f)] = dot(sv[rows(f)], wb[...])
            return carry

        lax.fori_loop(0, 2, stiff, 0)
        pl.when(it == 0)(lambda: pick(it))
        lax.fori_loop(2, 4, stiff, 0)
        await_picks(it)
        picks = [pk[...]] + [pkr[it, k] for k in range(4)]
        picks = jnp.concatenate(picks + [jnp.zeros((3 * PRIM, RHS), F32)], axis=0)
        high, low = halves(picks)
        pkhl[0:256] = high
        pkhl[256:512] = high
        pkhl[512:768] = low

        def complete(i, carry):
            f = 3 - i
            near = pl.ds(pl.multiple_of(PRIM * (f + 1), PRIM), PRIM)
            near_low = pl.ds(pl.multiple_of(PRIM * (f + 1) + 512, PRIM), PRIM)
            stack = jnp.concatenate(
                [pkhl[0:PRIM], pkhl[512 : 512 + PRIM], pkhl[near], pkhl[near_low]], axis=0
            )
            rank = dot(cmat[pl.ds(f, 1)].reshape(FACE, 128), stack)
            value = zz[pl.ds(it, 1), rows(f)].reshape(FACE, RHS) + rank
            zz[pl.ds(it, 1), rows(f)] = value[None]
            image = (
                t[rows(f)]
                + dot(sc[rows(f)], pkhl[0:512])
                + dot(sc[rows(f), 0:256], pkhl[512:768])
            )
            t[rows(f)] = image

            order_face(f, t)

            @pl.when(i < 2)
            def _():
                start_face(second, f, 0, CUT_STIFF)

            @pl.when(i >= 2)
            def _():
                start_face(second, f, 0, CUT_SIDE)

            wide = weight(f)
            acc[0] += wide * eighths(value * r[rows(f)])
            acc[1] += wide * eighths(value * q[rows(f)])
            acc[2] += eighths(image * value)
            acc[3] += eighths(image * zz[0, rows(f)])
            return carry

        lax.fori_loop(0, 4, complete, 0)
        for k in range(4):
            total = column_sums(acc[k])
            redz[k : k + 1] = total[:, 0:128]
            redz[4 + k : 5 + k] = total[:, 128:256]
        redzr[pl.ds(it, 1), pl.ds(g, 1)] = redz[...][None, None]

        def redz_copy(k):
            return pltpu.make_async_remote_copy(
                src_ref=redz,
                dst_ref=redzr.at[it, g],
                send_sem=redz_sem.at[it, 0],
                recv_sem=redz_sem.at[it, 1],
                device_id=((g + k) % ROWS, c),
                device_id_type=MESH,
            )

        for k in range(1, ROWS):
            redz_copy(k).start()
        pl.when(it == 0)(early_send)
        start_face(second, 3, CUT_STIFF, FACE)
        start_face(second, 2, CUT_STIFF, FACE)
        wait_bytes(
            redzr.at[it, pl.ds(0, ROWS - 1)], redz_sem.at[it, 0], redz_sem.at[it, 1], z_peer
        )
        red[...] = jnp.sum(redzr[pl.ds(it, 1)].reshape(ROWS, 8, 128), axis=0)

        def red_copy(k):
            return pltpu.make_async_remote_copy(
                src_ref=red,
                dst_ref=redr.at[it, c],
                send_sem=red_sem.at[it, 0],
                recv_sem=red_sem.at[it, 1],
                device_id=(g, (c + k) % COLS),
                device_id_type=MESH,
            )

        def start(k, carry):
            red_copy(k).start()
            return carry

        lax.fori_loop(1, COLS, start, 0)
        pl.when(it == 0)(early_launch)
        start_face(second, 1, CUT_SIDE, FACE)
        start_face(second, 0, CUT_SIDE, FACE)
        redr[pl.ds(it, 1), pl.ds(c, 1)] = red[...][None, None]
        wait_bytes(
            redr.at[it, pl.ds(0, COLS - 1)], red_sem.at[it, 0], red_sem.at[it, 1], row_peer
        )
        sums = jnp.sum(redr[pl.ds(it, 1)].reshape(COLS, 8, 128), axis=0)
        sums = jnp.concatenate([sums[0:4], sums[4:8]], axis=1)
        rz = sums[0:1]
        beta = jnp.where(it > 0, rz / scal[0:1], 0.0)
        curv = sums[2:3] + beta * (sums[1:2] + sums[3:4]) + beta * beta * scal[1:2]
        alpha = rz / curv
        scal[3:4] = scal[2:3]
        scal[0:1] = rz
        scal[1:2] = curv
        scal[2:3] = alpha
        scal[4:5] = beta

        def update(f, carry):
            await_face(second, f)
            image = t[rows(f)] + face_of(second, f) + beta * q[rows(f)]
            q[rows(f)] = image
            value = r[rows(f)] - alpha * image
            r[rows(f)] = value
            wb[rows(f)] = (value * weight(f)).astype(BF16)
            return carry

        lax.fori_loop(0, 4, update, 0)
        return carry

    lax.fori_loop(0, ITERS, step, 0)
    alpha = scal[2:3]
    held = scal[3:4] + alpha * scal[4:5]

    def finish(f, carry):
        t[rows(f)] = held * zz[0, rows(f)] + alpha * zz[1, rows(f)]
        return carry

    r_copy = pltpu.make_async_copy(r, r_out, out_sem.at[0])
    r_copy.start()
    lax.fori_loop(0, 4, finish, 0)
    x_copy = pltpu.make_async_copy(t, x_out, out_sem.at[1])
    x_copy.start()
    r_copy.wait()
    x_copy.wait()


def body(
    load, schur, local_inverse, face_map, primal_basis, primal_index,
    group_inverse, group_to_coarsest, coarsest_inverse,
):
    anywhere = pl.BlockSpec(memory_space=pl.ANY)
    near = pl.BlockSpec(memory_space=pltpu.VMEM)
    dma = pltpu.SemaphoreType.DMA
    out = jax.ShapeDtypeStruct((IFACE, RHS), F32)
    x, r = pl.pallas_call(
        kernel,
        out_shape=(out, out),
        in_specs=[anywhere] * 3 + [near] * 6,
        out_specs=(anywhere, anywhere),
        scratch_shapes=[
            pltpu.VMEM((IFACE, IFACE), BF16),
            pltpu.VMEM((IFACE, IFACE), BF16),
            pltpu.VMEM((IFACE, RHS), F32),
            pltpu.VMEM((IFACE, RHS), F32),
            pltpu.VMEM((IFACE, RHS), F32),
            pltpu.VMEM((ITERS, IFACE, RHS), F32),
            pltpu.VMEM((IFACE, RHS), BF16),
            pltpu.VMEM((4, FACE, FACE), BF16),
            pltpu.VMEM((4, FACE, RHS), F32),
            pltpu.VMEM((1 + 2 * ITERS, 4, FACE, RHS), F32),
            pltpu.VMEM((4, FACE, 128), BF16),
            pltpu.VMEM((4, PRIM, FACE), F32),
            pltpu.VMEM((4, PRIM, FACE), F32),
            pltpu.VMEM((8, 128), F32),
            pltpu.VMEM((COLS, 8, 128), F32),
            pltpu.VMEM((COLS, BLOCK, NQ), F32),
            pltpu.VMEM((4, BLOCK, NCG), F32),
            pltpu.VMEM((NCG, NCG), BF16),
            pltpu.VMEM((NCG, 128), BF16),
            pltpu.VMEM((256, NCG), BF16),
            pltpu.VMEM((256, NCG), BF16),
            pltpu.VMEM((PRIM, NQ), F32),
            pltpu.VMEM((NCG, 128), F32),
            pltpu.VMEM((IFACE, 256), BF16),
            pltpu.VMEM((IFACE, 512), BF16),
            pltpu.VMEM((64, 128), F32),
            pltpu.VMEM((ITERS, 4, 64, 128), F32),
            pltpu.VMEM((768, RHS), BF16),
            pltpu.VMEM((4, 16, 128), F32),
            pltpu.VMEM((ITERS, COLS, 16, 128), F32),
            pltpu.VMEM((64, 128), F32),
            pltpu.VMEM((ITERS, ROWS, 64, 128), F32),
            pltpu.VMEM((COLS, 16, 128), F32),
            pltpu.VMEM((ITERS, COLS, 16, 128), F32),
            pltpu.VMEM((PRIM, RHS), F32),
            pltpu.VMEM((ITERS, 4, PRIM, RHS), F32),
            pltpu.VMEM((8, 128), F32),
            pltpu.VMEM((ITERS, COLS, 8, 128), F32),
            pltpu.VMEM((8, 128), F32),
            pltpu.VMEM((ITERS, ROWS, 8, 128), F32),
            pltpu.VMEM((4, 8, RHS), F32),
            pltpu.VMEM((8, RHS), F32),
            pltpu.VMEM((4, 2 * PRIM, FACE), BF16),
            pltpu.VMEM((4, PRIM, RHS), F32),
            pltpu.VMEM((4, PRIM, RHS), F32),
            pltpu.VMEM((PRIM, RHS), F32),
            pltpu.VMEM((PRIM, RHS), F32),
            dma((4,)), dma((2,)), dma((4,)), dma((1 + 2 * ITERS, 4)),
            dma((4,)), dma((4,)), dma((2,)), dma((2,)), dma((2,)),
            dma((ITERS, 2)), dma((ITERS, 2)), dma((ITERS, 2)), dma((ITERS, 2)),
            dma((4,)), dma((ITERS, 4)), dma((ITERS, 2)), dma((ITERS, 2)), dma((2,)),
            dma((4,)), dma((4,)),
        ],
        compiler_params=pltpu.CompilerParams(
            collective_id=0, has_side_effects=True, vmem_limit_bytes=63 * 1024 * 1024
        ),
    )(
        load[0], schur[0], local_inverse[0], face_map[0], primal_basis[0], primal_index,
        group_inverse[0], group_to_coarsest[0], coarsest_inverse,
    )
    return x[None], r[None]


def solution(mesh):
    spread = ("grp", "cell")
    in_specs = (
        P(spread, None, None),
        P(spread, None, None),
        P(spread, None, None),
        P(spread, None, None),
        P(spread, None, None),
        P(spread, None),
        P("grp", "cell", None),
        P("grp", "cell", None),
        P(),
    )
    out_specs = (P(spread, None, None), P(spread, None, None))
    return jax.shard_map(body, mesh=mesh, in_specs=in_specs, out_specs=out_specs, check_vma=False)
```

```python
import jax
import jax.numpy as jnp
from jax import lax
from jax.experimental import pallas as pl
from jax.experimental.pallas import tpu as pltpu
from jax.sharding import PartitionSpec as P

MESH = pl.DeviceIdType.MESH
HIGHEST = lax.Precision.HIGHEST
F32 = jnp.float32
BF16 = jnp.bfloat16

ROWS = 4
COLS = 32
IFACE = 2048
FACE = 512
RHS = 256
PRIM = 32
NQ = 128
NCG = 1024
ITERS = 2
BLOCK = NCG // COLS
CUT_LOCAL = 384
CUT_AGAIN = 128
CUT_STIFF = 160
CUT_SIDE = 256


def dot(a, b):
    return jnp.dot(a, b, preferred_element_type=F32)


def halves(value):
    high = value.astype(BF16)
    return high, (value - high.astype(F32)).astype(BF16)


def column_sums(value):
    return jnp.sum(value, axis=0, keepdims=True)


def eighths(value):
    return jnp.sum(value.reshape(FACE // 8, 8, RHS), axis=0)


def kernel(
    load_h, schur_h, linv_h, fmap, basis, index, ginv, lifting, cinv,
    x_out, r_out,
    sv, lv, r, t, q, zz, wb, perm, send, recv, cmat, nbsend, nbrecv,
    myspots, prow, srecv, gin, et, fm, whi, wlo, egc, gc, chat, sc, css, csr, pkhl,
    pbuf, xrecv, zcs, zcr, obuf, orecv, pk, pkr, red, redr, redz, redzr, acc, scal,
    pmat, ems, emr, pq, pkb,
    load_sem, mat_sem, face_ssem, face_rsem, nb_ssem, nb_rsem, spot_sem, set_sem, gin_sem,
    x_sem, zc_sem, cs_sem, o_sem, pk_ssem, pk_rsem, red_sem, redz_sem, out_sem, em_ssem, em_rsem,
):
    g = lax.axis_index("grp")
    c = lax.axis_index("cell")
    xq = c // 8
    rest = c % 8

    def rows(f):
        return pl.ds(pl.multiple_of(f * FACE, FACE), FACE)

    def where_is(f):
        axis = f // 2
        sign = 2 * (f % 2) - 1
        gg = g + axis * sign
        cc = c + (1 - axis) * sign
        exists = jnp.logical_and(
            jnp.logical_and(gg >= 0, gg < ROWS), jnp.logical_and(cc >= 0, cc < COLS)
        )
        return exists, (gg, cc)

    def weight(f):
        exists, _ = where_is(f)
        return jnp.where(exists, 0.5, 1.0).astype(F32)

    def other(f):
        return f + 1 - 2 * (f % 2)

    load_copies = [
        pltpu.make_async_copy(
            load_h.at[pl.ds(f * FACE, FACE)], r.at[pl.ds(f * FACE, FACE)], load_sem.at[f]
        )
        for f in range(4)
    ]
    for f in (3, 2, 1, 0):
        load_copies[f].start()
    linv_copy = pltpu.make_async_copy(linv_h, lv, mat_sem.at[0])
    schur_copy = pltpu.make_async_copy(schur_h, sv, mat_sem.at[1])

    barrier = pltpu.get_barrier_semaphore()

    def greet_row(k, carry):
        pl.semaphore_signal(
            barrier, inc=1, device_id=(g, (c + k) % COLS), device_id_type=MESH
        )
        return carry

    lax.fori_loop(1, COLS, greet_row, 0)
    for k in range(1, ROWS):
        pl.semaphore_signal(
            barrier, inc=1, device_id=((g + k) % ROWS, c), device_id_type=MESH
        )

    def build_perm(f, carry):
        mine = fmap[pl.ds(f, 1), :]
        places = lax.broadcasted_iota(jnp.int32, (FACE, FACE), 0)
        perm[pl.ds(f, 1)] = jnp.where(places == mine, 1.0, 0.0).astype(BF16)[None]
        return carry

    lax.fori_loop(0, 4, build_perm, 0)

    def face_copy(e, f, start, stop):
        _, there = where_is(f)
        return pltpu.make_async_remote_copy(
            src_ref=send.at[f, pl.ds(start, stop - start)],
            dst_ref=recv.at[e, other(f), pl.ds(start, stop - start)],
            send_sem=face_ssem.at[f],
            recv_sem=face_rsem.at[e, other(f)],
            device_id=there,
            device_id_type=MESH,
        )

    def face_arrival(e, f):
        _, there = where_is(f)
        return pltpu.make_async_remote_copy(
            src_ref=send.at[f],
            dst_ref=recv.at[e, f],
            send_sem=face_ssem.at[f],
            recv_sem=face_rsem.at[e, f],
            device_id=there,
            device_id_type=MESH,
        )

    def order_face(f, ref):
        exists, _ = where_is(f)

        @pl.when(exists)
        def _():
            high, low = halves(ref[rows(f)])
            order = perm[pl.ds(f, 1)].reshape(FACE, FACE)
            send[pl.ds(f, 1)] = (dot(order, high) + dot(order, low))[None]

    def start_face(e, f, start, stop):
        exists, _ = where_is(f)

        @pl.when(exists)
        def _():
            face_copy(e, f, start, stop).start()

    def await_face(e, f):
        exists, _ = where_is(f)

        @pl.when(exists)
        def _():
            arrival = face_arrival(e, f)
            arrival.wait_recv()
            arrival.wait_send()

        @pl.when(jnp.logical_not(exists))
        def _():
            recv[pl.ds(e, 1), pl.ds(f, 1)] = jnp.zeros((1, 1, FACE, RHS), F32)

    def face_of(e, f):
        return recv[pl.ds(e, 1), pl.ds(f, 1)].reshape(FACE, RHS)

    for f in (3, 2, 1, 0):
        load_copies[f].wait()
        if f == 3:
            linv_copy.start()
            schur_copy.start()
        order_face(f, r)

    lane = lax.broadcasted_iota(jnp.int32, (PRIM, 128), 1)
    line = lax.broadcasted_iota(jnp.int32, (PRIM, 128), 0)
    spots = jnp.broadcast_to(index[...].astype(F32), (8, PRIM))
    low_spots = jnp.dot(
        spots, jnp.where(line == lane % 16, 1.0, 0.0).astype(F32),
        precision=HIGHEST, preferred_element_type=F32,
    )
    high_spots = jnp.dot(
        spots, jnp.where(line == lane % 16 + 16, 1.0, 0.0).astype(F32),
        precision=HIGHEST, preferred_element_type=F32,
    )
    first_line = lax.broadcasted_iota(jnp.int32, (8, 128), 0) == 0
    myspots[...] = jnp.where(first_line, low_spots, high_spots)
    prow[pl.ds(c, 1)] = myspots[...][None]
    srecv[pl.ds(c, 1)] = lifting[...][None]
    gin[pl.ds(xq, 1)] = ginv[...][None]

    pl.semaphore_wait(barrier, COLS - 1 + ROWS - 1)
    start_face(0, 3, 0, FACE)
    start_face(0, 2, 0, FACE)

    def spots_copy(k):
        return pltpu.make_async_remote_copy(
            src_ref=myspots,
            dst_ref=prow.at[c],
            send_sem=spot_sem.at[0],
            recv_sem=spot_sem.at[1],
            device_id=(g, (c + k) % COLS),
            device_id_type=MESH,
        )

    def start_spots(k, carry):
        spots_copy(k).start()
        return carry

    lax.fori_loop(1, COLS, start_spots, 0)
    start_face(0, 1, 0, FACE)
    start_face(0, 0, 0, FACE)

    def setup_copy(k):
        return pltpu.make_async_remote_copy(
            src_ref=lifting,
            dst_ref=srecv.at[c],
            send_sem=set_sem.at[0],
            recv_sem=set_sem.at[1],
            device_id=(g, (c + k) % COLS),
            device_id_type=MESH,
        )

    def start_setup(k, carry):
        setup_copy(k).start()
        return carry

    def gin_copy(k):
        return pltpu.make_async_remote_copy(
            src_ref=ginv,
            dst_ref=gin.at[xq],
            send_sem=gin_sem.at[0],
            recv_sem=gin_sem.at[1],
            device_id=(g, ((xq + k) % 4) * 8 + rest),
            device_id_type=MESH,
        )

    for k in range(1, 4):
        gin_copy(k).start()
    lax.fori_loop(1, COLS, start_setup, 0)

    def nb_copy(f, slot):
        _, there = where_is(f)
        return pltpu.make_async_remote_copy(
            src_ref=nbsend.at[f],
            dst_ref=nbrecv.at[slot],
            send_sem=nb_ssem.at[f],
            recv_sem=nb_rsem.at[slot],
            device_id=there,
            device_id_type=MESH,
        )

    for f in range(4):
        exists, _ = where_is(f)

        @pl.when(exists)
        def _():
            nbsend[f] = lax.dot_general(
                basis[:, f * FACE : (f + 1) * FACE], perm[f],
                (((1,), (1,)), ((), ())), preferred_element_type=F32,
            )
            nb_copy(f, f ^ 1).start()

        @pl.when(jnp.logical_not(exists))
        def _():
            nbrecv[f] = jnp.zeros((PRIM, FACE), F32)
            pkr[0, f] = jnp.zeros((PRIM, RHS), F32)
            pkr[1, f] = jnp.zeros((PRIM, RHS), F32)
            emr[f] = jnp.zeros((PRIM, RHS), F32)

    q[...] = jnp.zeros_like(q)
    scal[...] = jnp.ones_like(scal)

    def wait_bytes(ref, ssem, rsem, to):
        both = pltpu.make_async_remote_copy(
            src_ref=ref, dst_ref=ref, send_sem=ssem, recv_sem=rsem,
            device_id=to, device_id_type=MESH,
        )
        both.wait_recv()
        both.wait_send()

    row_peer = (g, (c + 1) % COLS)
    z_peer = ((g + 1) % ROWS, c)

    wait_bytes(prow.at[pl.ds(0, COLS - 1)], spot_sem.at[0], spot_sem.at[1], row_peer)

    lane1 = lax.broadcasted_iota(jnp.int32, (1, 128), 1)

    def spots_of(line_number):
        parts = []
        for quarter in range(4):
            total = jnp.zeros((1, 128), F32)
            for n in range(8 * quarter, 8 * quarter + 8):
                row = prow[n, line_number : line_number + 1, :]
                total = total + jnp.where(lane1 // 16 == n % 8, row, 0.0)
            parts.append(total)
        return jnp.concatenate(parts, axis=1).astype(jnp.int32)

    wanted = jnp.concatenate([spots_of(0), spots_of(1)], axis=1)

    for block in range(8):
        target = lax.broadcasted_iota(jnp.int32, (128, NCG), 0) + block * 128
        et[pl.ds(block * 128, 128)] = jnp.where(target == wanted, 1.0, 0.0).astype(BF16)

    own_row = lax.broadcasted_iota(jnp.int32, (128, NCG), 0)
    own_row = (own_row // BLOCK) * (8 * BLOCK) + rest * BLOCK + own_row % BLOCK
    fm[...] = jnp.where(own_row == wanted, 1.0, 0.0).astype(F32).T.astype(BF16)

    wait_bytes(gin.at[pl.ds(0, 3)], gin_sem.at[0], gin_sem.at[1], row_peer)
    high, low = halves(gin[...].reshape(128, NCG))
    whi[0:128] = high
    wlo[0:128] = low

    def build_late():
        wait_bytes(srecv.at[pl.ds(0, COLS - 1)], set_sem.at[0], set_sem.at[1], row_peer)
        all_lifting = srecv[...].reshape(NCG, NQ)
        high, low = halves(all_lifting.T)
        whi[128:256] = high
        wlo[128:256] = low
        mine = jnp.where(lane1 < 16, myspots[0:1], myspots[1:2]).astype(jnp.int32)
        target = lax.broadcasted_iota(jnp.int32, (NCG, 128), 0)
        chosen = jnp.where(target == mine, 1.0, 0.0).astype(F32).T[0:PRIM].astype(BF16)
        high, low = halves(all_lifting)
        egc[...] = jnp.dot(
            dot(chosen, high) + dot(chosen, low), cinv[...],
            precision=HIGHEST, preferred_element_type=F32,
        )

    def build_rank():
        for f in range(4):
            exists, _ = where_is(f)

            @pl.when(exists)
            def _():
                both = nb_copy(f, f)
                both.wait_recv()
                both.wait_send()

            own = basis[:, f * FACE : (f + 1) * FACE].astype(F32)
            near = nbrecv[f]
            stack = jnp.concatenate([own, own, near, near], axis=0) * weight(f)
            cmat[f] = stack.T.astype(BF16)
            pmat[f] = (jnp.concatenate([own, near], axis=0) * weight(f)).astype(BF16)
            empty = jnp.zeros((PRIM, FACE), F32)
            stack = jnp.concatenate(
                [own] + [near if k == f else empty for k in range(4)] + [empty] * 3, axis=0
            )
            chat[f * FACE : (f + 1) * FACE] = (stack * weight(f)).T.astype(BF16)

        def build_images(f, carry):
            high, low = halves(dot(sv[rows(f)], chat[...]))
            sc[rows(f), 0:256] = high
            sc[rows(f), 256:512] = low
            return carry

        lax.fori_loop(0, 4, build_images, 0)

    linv_copy.wait()
    schur_copy.wait()

    def settle_start(i, carry):
        await_face(0, i)
        value = r[rows(i)] + face_of(0, i)
        r[rows(i)] = value
        wb[rows(i)] = (value * weight(i)).astype(BF16)
        return carry

    lax.fori_loop(0, 4, settle_start, 0)

    lane_wide = lax.broadcasted_iota(jnp.int32, (16, 128), 1)

    def left(shape):
        return lax.broadcasted_iota(jnp.int32, shape, 1) < 64

    def swap(value):
        return pltpu.roll(value, 64, 1)

    def coarse(it, primal):
        def x_copy(k):
            there = (c + k) % COLS
            return pltpu.make_async_remote_copy(
                src_ref=pbuf.at[there // 8],
                dst_ref=xrecv.at[it, c],
                send_sem=x_sem.at[it, 0],
                recv_sem=x_sem.at[it, 1],
                device_id=(g, there),
                device_id_type=MESH,
            )

        for pair in range(2):
            part = primal[:, 128 * pair : 128 * pair + 128]
            top, bottom = part[0:16], part[16:32]
            pbuf[2 * pair] = jnp.where(lane_wide < 64, top, swap(bottom))
            pbuf[2 * pair + 1] = jnp.where(lane_wide < 64, swap(top), bottom)

        def start(k, carry):
            x_copy(k).start()
            return carry

        lax.fori_loop(1, COLS, start, 0)
        xrecv[pl.ds(it, 1), pl.ds(c, 1)] = pbuf[pl.ds(xq, 1)][None]

    def unpack(blocks, half):
        columns = []
        lanes = left((half, 128))
        for pair in range(2):
            first, second = blocks[2 * pair], blocks[2 * pair + 1]
            top = jnp.where(lanes, first, swap(second))
            bottom = jnp.where(lanes, swap(first), second)
            columns.append(jnp.concatenate([top, bottom], axis=0))
        return jnp.concatenate(columns, axis=1)

    def solve_row(it, cut):
        wait_bytes(xrecv.at[it, pl.ds(0, COLS - 1)], x_sem.at[it, 0], x_sem.at[it, 1], row_peer)
        block = xrecv[pl.ds(it, 1)].reshape(FACE, 128)
        parts = jnp.concatenate(halves(block), axis=1)
        upper = dot(et[:, 0:512], parts)
        lower = dot(et[:, 512:1024], parts)
        upper = upper[:, 0:128] + upper[:, 128:256]
        lower = lower[:, 0:128] + lower[:, 128:256]
        gc[...] = upper + swap(lower)
        high, low = halves(gc[...])
        both = dot(whi[...], jnp.concatenate([high, low], axis=1))
        both = both[:, 0:128] + both[:, 128:256] + dot(wlo[...], high)
        partial = both[128:256]
        packed = jnp.where(left((64, 128)), partial[0:64], swap(partial[64:128]))
        zcs[...] = packed
        zcr[pl.ds(it, 1), pl.ds(g, 1)] = packed[None, None]

        def z_copy(k):
            return pltpu.make_async_remote_copy(
                src_ref=zcs,
                dst_ref=zcr.at[it, g],
                send_sem=zc_sem.at[it, 0],
                recv_sem=zc_sem.at[it, 1],
                device_id=((g + k) % ROWS, c),
                device_id_type=MESH,
            )

        for k in range(1, ROWS):
            z_copy(k).start()
        start_face(1 + 2 * it, 3, cut, FACE)
        start_face(1 + 2 * it, 2, cut, FACE)
        parts = jnp.concatenate(halves(both[0:128]), axis=1)
        back = dot(fm[...], parts)
        back = back[:, 0:128] + back[:, 128:256]
        packed = jnp.where(left((FACE, 128)), back[0:512], swap(back[512:1024]))
        obuf[...] = packed.reshape(COLS, 16, 128)

        def o_copy(k):
            there = (c + k) % COLS
            return pltpu.make_async_remote_copy(
                src_ref=obuf.at[there],
                dst_ref=orecv.at[it, c],
                send_sem=o_sem.at[it, 0],
                recv_sem=o_sem.at[it, 1],
                device_id=(g, there),
                device_id_type=MESH,
            )

        def start(k, carry):
            o_copy(k).start()
            return carry

        lax.fori_loop(1, COLS, start, 0)
        orecv[pl.ds(it, 1), pl.ds(c, 1)] = obuf[pl.ds(c, 1)][None]

    def solve_coarsest(it):
        wait_bytes(zcr.at[it, pl.ds(0, ROWS - 1)], zc_sem.at[it, 0], zc_sem.at[it, 1], z_peer)
        blocks = zcr[pl.ds(it, 1)].reshape(ROWS, 64, 128)
        total = (blocks[0] + blocks[1]) + (blocks[2] + blocks[3])
        css[...] = total
        csr[pl.ds(it, 1), pl.ds(xq, 1)] = total[None, None]

        def cs_copy(k):
            return pltpu.make_async_remote_copy(
                src_ref=css,
                dst_ref=csr.at[it, xq],
                send_sem=cs_sem.at[it, 0],
                recv_sem=cs_sem.at[it, 1],
                device_id=(g, ((xq + k) % 4) * 8 + rest),
                device_id_type=MESH,
            )

        for k in range(1, 4):
            cs_copy(k).start()

    def pk_copy(it, f, slot):
        _, there = where_is(f)
        return pltpu.make_async_remote_copy(
            src_ref=pk,
            dst_ref=pkr.at[it, slot],
            send_sem=pk_ssem.at[f],
            recv_sem=pk_rsem.at[it, slot],
            device_id=there,
            device_id_type=MESH,
        )

    def pick(it):
        wait_bytes(csr.at[it, pl.ds(0, 3)], cs_sem.at[it, 0], cs_sem.at[it, 1], row_peer)
        coarsest = unpack([csr[it, k] for k in range(4)], 64)
        wait_bytes(orecv.at[it, pl.ds(0, COLS - 1)], o_sem.at[it, 0], o_sem.at[it, 1], row_peer)
        sums = jnp.sum(orecv[pl.ds(it, 1)].reshape(4, 8, 16, 128), axis=1)
        found = unpack([sums[k] for k in range(4)], 16) + jnp.dot(
            egc[...], coarsest, precision=HIGHEST, preferred_element_type=F32
        )

        @pl.when(it == 0)
        def _():
            pk[...] = found
            pkb[...] = found

        @pl.when(it > 0)
        def _():
            pk[...] = pkb[...] - scal[2:3] * found

        for f in range(4):
            exists, _ = where_is(f)

            @pl.when(exists)
            def _():
                pk_copy(it, f, f ^ 1).start()

    def await_picks(it):
        for f in range(4):
            exists, _ = where_is(f)

            @pl.when(exists)
            def _():
                arrival = pk_copy(it, f, f)
                arrival.wait_recv()
                arrival.wait_send()

    def em_copy(f, slot):
        _, there = where_is(f)
        return pltpu.make_async_remote_copy(
            src_ref=ems.at[f],
            dst_ref=emr.at[slot],
            send_sem=em_ssem.at[f],
            recv_sem=em_rsem.at[slot],
            device_id=there,
            device_id_type=MESH,
        )

    def early_send():
        pq[...] = jnp.zeros_like(pq)

        def one(i, carry):
            f = 3 - i
            both = dot(pmat[pl.ds(f, 1)].reshape(2 * PRIM, FACE), jnp.concatenate(
                halves(t[rows(f)]), axis=1
            ))
            both = both[:, 0:RHS] + both[:, RHS:]
            pq[...] += both[0:PRIM]
            ems[pl.ds(f, 1)] = both[PRIM:][None]
            exists, _ = where_is(f)

            @pl.when(exists)
            def _():
                em_copy(f, other(f)).start()

            return carry

        lax.fori_loop(0, 4, one, 0)

    def early_launch():
        for f in range(4):
            exists, _ = where_is(f)

            @pl.when(exists)
            def _():
                arrival = em_copy(f, f)
                arrival.wait_recv()
                arrival.wait_send()

        coarse(1, pq[...] + ((emr[0] + emr[1]) + (emr[2] + emr[3])))

    x_copy = pltpu.make_async_copy(zz.at[0], x_out, out_sem.at[4])

    def r_copy(f):
        return pltpu.make_async_copy(r.at[rows(f)], r_out.at[rows(f)], out_sem.at[f])

    def step(it, carry):
        acc[...] = jnp.zeros_like(acc)
        first = 1 + 2 * it
        second = 2 + 2 * it

        pl.when(it == 0)(lambda: coarse(0, dot(basis[...], wb[...])))

        def local(i, carry):
            f = 3 - i
            t[rows(f)] = dot(lv[rows(f)], wb[...]) * weight(f)
            order_face(f, t)

            @pl.when(jnp.logical_and(i < 2, it == 0))
            def _():
                start_face(first, f, 0, CUT_LOCAL)

            @pl.when(jnp.logical_and(i < 2, it > 0))
            def _():
                start_face(first, f, 0, CUT_AGAIN)

            @pl.when(i >= 2)
            def _():
                start_face(first, f, 0, FACE)

            return carry

        lax.fori_loop(0, 2, local, 0)
        pl.when(it > 0)(lambda: solve_row(1, CUT_AGAIN))
        lax.fori_loop(2, 4, local, 0)

        @pl.when(it == 0)
        def _():
            build_late()
            solve_row(0, CUT_LOCAL)
            build_rank()

        solve_coarsest(it)
        pl.when(it > 0)(lambda: pick(it))

        def settle(f, carry):
            await_face(first, f)
            value = t[rows(f)] + face_of(first, f)
            zz[pl.ds(it, 1), rows(f)] = value[None]
            wb[rows(f)] = value.astype(BF16)
            return carry

        lax.fori_loop(0, 4, settle, 0)

        def stiff(i, carry):
            f = 3 - i
            t[rows(f)] = dot(sv[rows(f)], wb[...])
            return carry

        lax.fori_loop(0, 2, stiff, 0)
        pl.when(it == 0)(lambda: pick(it))
        lax.fori_loop(2, 4, stiff, 0)
        await_picks(it)
        picks = [pk[...]] + [pkr[it, k] for k in range(4)]
        picks = jnp.concatenate(picks + [jnp.zeros((3 * PRIM, RHS), F32)], axis=0)
        high, low = halves(picks)
        pkhl[0:256] = high
        pkhl[256:512] = high
        pkhl[512:768] = low

        def complete(i, carry):
            f = 3 - i
            near = pl.ds(pl.multiple_of(PRIM * (f + 1), PRIM), PRIM)
            near_low = pl.ds(pl.multiple_of(PRIM * (f + 1) + 512, PRIM), PRIM)
            stack = jnp.concatenate(
                [pkhl[0:PRIM], pkhl[512 : 512 + PRIM], pkhl[near], pkhl[near_low]], axis=0
            )
            rank = dot(cmat[pl.ds(f, 1)].reshape(FACE, 128), stack)
            value = zz[pl.ds(it, 1), rows(f)].reshape(FACE, RHS) + rank
            zz[pl.ds(it, 1), rows(f)] = value[None]
            image = (
                t[rows(f)]
                + dot(sc[rows(f)], pkhl[0:512])
                + dot(sc[rows(f), 0:256], pkhl[512:768])
            )
            t[rows(f)] = image

            order_face(f, t)

            @pl.when(i < 2)
            def _():
                start_face(second, f, 0, CUT_STIFF)

            @pl.when(i >= 2)
            def _():
                start_face(second, f, 0, CUT_SIDE)

            wide = weight(f)
            acc[0] += wide * eighths(value * r[rows(f)])
            acc[1] += wide * eighths(value * q[rows(f)])
            acc[2] += eighths(image * value)
            acc[3] += eighths(image * zz[0, rows(f)])
            return carry

        lax.fori_loop(0, 4, complete, 0)
        for k in range(4):
            total = column_sums(acc[k])
            redz[k : k + 1] = total[:, 0:128]
            redz[4 + k : 5 + k] = total[:, 128:256]
        redzr[pl.ds(it, 1), pl.ds(g, 1)] = redz[...][None, None]

        def redz_copy(k):
            return pltpu.make_async_remote_copy(
                src_ref=redz,
                dst_ref=redzr.at[it, g],
                send_sem=redz_sem.at[it, 0],
                recv_sem=redz_sem.at[it, 1],
                device_id=((g + k) % ROWS, c),
                device_id_type=MESH,
            )

        for k in range(1, ROWS):
            redz_copy(k).start()
        pl.when(it == 0)(early_send)
        start_face(second, 3, CUT_STIFF, FACE)
        start_face(second, 2, CUT_STIFF, FACE)
        wait_bytes(
            redzr.at[it, pl.ds(0, ROWS - 1)], redz_sem.at[it, 0], redz_sem.at[it, 1], z_peer
        )
        red[...] = jnp.sum(redzr[pl.ds(it, 1)].reshape(ROWS, 8, 128), axis=0)

        def red_copy(k):
            return pltpu.make_async_remote_copy(
                src_ref=red,
                dst_ref=redr.at[it, c],
                send_sem=red_sem.at[it, 0],
                recv_sem=red_sem.at[it, 1],
                device_id=(g, (c + k) % COLS),
                device_id_type=MESH,
            )

        def start(k, carry):
            red_copy(k).start()
            return carry

        lax.fori_loop(1, COLS, start, 0)
        pl.when(it == 0)(early_launch)
        start_face(second, 1, CUT_SIDE, FACE)
        start_face(second, 0, CUT_SIDE, FACE)
        redr[pl.ds(it, 1), pl.ds(c, 1)] = red[...][None, None]
        wait_bytes(
            redr.at[it, pl.ds(0, COLS - 1)], red_sem.at[it, 0], red_sem.at[it, 1], row_peer
        )
        sums = jnp.sum(redr[pl.ds(it, 1)].reshape(COLS, 8, 128), axis=0)
        sums = jnp.concatenate([sums[0:4], sums[4:8]], axis=1)
        rz = sums[0:1]
        beta = jnp.where(it > 0, rz / scal[0:1], 0.0)
        curv = sums[2:3] + beta * (sums[1:2] + sums[3:4]) + beta * beta * scal[1:2]
        alpha = rz / curv
        scal[3:4] = scal[2:3]
        scal[0:1] = rz
        scal[1:2] = curv
        scal[2:3] = alpha
        scal[4:5] = beta

        @pl.when(it == ITERS - 1)
        def _():
            held = scal[3:4] + alpha * beta

            def finish(f, carry):
                zz[0, rows(f)] = held * zz[0, rows(f)] + alpha * zz[1, rows(f)]
                return carry

            lax.fori_loop(0, 4, finish, 0)
            x_copy.start()


        def update(f, carry):
            await_face(second, f)
            image = t[rows(f)] + face_of(second, f) + beta * q[rows(f)]
            q[rows(f)] = image
            value = r[rows(f)] - alpha * image
            r[rows(f)] = value
            wb[rows(f)] = (value * weight(f)).astype(BF16)

            @pl.when(it == ITERS - 1)
            def _():
                r_copy(f).start()

            return carry

        lax.fori_loop(0, 4, update, 0)
        return carry

    lax.fori_loop(0, ITERS, step, 0)
    for f in range(4):
        r_copy(f).wait()
    x_copy.wait()


def body(
    load, schur, local_inverse, face_map, primal_basis, primal_index,
    group_inverse, group_to_coarsest, coarsest_inverse,
):
    anywhere = pl.BlockSpec(memory_space=pl.ANY)
    near = pl.BlockSpec(memory_space=pltpu.VMEM)
    dma = pltpu.SemaphoreType.DMA
    out = jax.ShapeDtypeStruct((IFACE, RHS), F32)
    x, r = pl.pallas_call(
        kernel,
        out_shape=(out, out),
        in_specs=[anywhere] * 3 + [near] * 6,
        out_specs=(anywhere, anywhere),
        scratch_shapes=[
            pltpu.VMEM((IFACE, IFACE), BF16),
            pltpu.VMEM((IFACE, IFACE), BF16),
            pltpu.VMEM((IFACE, RHS), F32),
            pltpu.VMEM((IFACE, RHS), F32),
            pltpu.VMEM((IFACE, RHS), F32),
            pltpu.VMEM((ITERS, IFACE, RHS), F32),
            pltpu.VMEM((IFACE, RHS), BF16),
            pltpu.VMEM((4, FACE, FACE), BF16),
            pltpu.VMEM((4, FACE, RHS), F32),
            pltpu.VMEM((1 + 2 * ITERS, 4, FACE, RHS), F32),
            pltpu.VMEM((4, FACE, 128), BF16),
            pltpu.VMEM((4, PRIM, FACE), F32),
            pltpu.VMEM((4, PRIM, FACE), F32),
            pltpu.VMEM((8, 128), F32),
            pltpu.VMEM((COLS, 8, 128), F32),
            pltpu.VMEM((COLS, BLOCK, NQ), F32),
            pltpu.VMEM((4, BLOCK, NCG), F32),
            pltpu.VMEM((NCG, NCG), BF16),
            pltpu.VMEM((NCG, 128), BF16),
            pltpu.VMEM((256, NCG), BF16),
            pltpu.VMEM((256, NCG), BF16),
            pltpu.VMEM((PRIM, NQ), F32),
            pltpu.VMEM((NCG, 128), F32),
            pltpu.VMEM((IFACE, 256), BF16),
            pltpu.VMEM((IFACE, 512), BF16),
            pltpu.VMEM((64, 128), F32),
            pltpu.VMEM((ITERS, 4, 64, 128), F32),
            pltpu.VMEM((768, RHS), BF16),
            pltpu.VMEM((4, 16, 128), F32),
            pltpu.VMEM((ITERS, COLS, 16, 128), F32),
            pltpu.VMEM((64, 128), F32),
            pltpu.VMEM((ITERS, ROWS, 64, 128), F32),
            pltpu.VMEM((COLS, 16, 128), F32),
            pltpu.VMEM((ITERS, COLS, 16, 128), F32),
            pltpu.VMEM((PRIM, RHS), F32),
            pltpu.VMEM((ITERS, 4, PRIM, RHS), F32),
            pltpu.VMEM((8, 128), F32),
            pltpu.VMEM((ITERS, COLS, 8, 128), F32),
            pltpu.VMEM((8, 128), F32),
            pltpu.VMEM((ITERS, ROWS, 8, 128), F32),
            pltpu.VMEM((4, 8, RHS), F32),
            pltpu.VMEM((8, RHS), F32),
            pltpu.VMEM((4, 2 * PRIM, FACE), BF16),
            pltpu.VMEM((4, PRIM, RHS), F32),
            pltpu.VMEM((4, PRIM, RHS), F32),
            pltpu.VMEM((PRIM, RHS), F32),
            pltpu.VMEM((PRIM, RHS), F32),
            dma((4,)), dma((2,)), dma((4,)), dma((1 + 2 * ITERS, 4)),
            dma((4,)), dma((4,)), dma((2,)), dma((2,)), dma((2,)),
            dma((ITERS, 2)), dma((ITERS, 2)), dma((ITERS, 2)), dma((ITERS, 2)),
            dma((4,)), dma((ITERS, 4)), dma((ITERS, 2)), dma((ITERS, 2)), dma((5,)),
            dma((4,)), dma((4,)),
        ],
        compiler_params=pltpu.CompilerParams(
            collective_id=0, has_side_effects=True, vmem_limit_bytes=63 * 1024 * 1024
        ),
    )(
        load[0], schur[0], local_inverse[0], face_map[0], primal_basis[0], primal_index,
        group_inverse[0], group_to_coarsest[0], coarsest_inverse,
    )
    return x[None], r[None]


def solution(mesh):
    spread = ("grp", "cell")
    in_specs = (
        P(spread, None, None),
        P(spread, None, None),
        P(spread, None, None),
        P(spread, None, None),
        P(spread, None, None),
        P(spread, None),
        P("grp", "cell", None),
        P("grp", "cell", None),
        P(),
    )
    out_specs = (P(spread, None, None), P(spread, None, None))
    return jax.shard_map(body, mesh=mesh, in_specs=in_specs, out_specs=out_specs, check_vma=False)
```
